256 devices in a mesh: walk: 32 (over z, x), chol: 8 (over y, core).
Axes of the slice: x: 4, y: 4, z: 8, core: 2. Of those that a mesh axis runs over, the one named last changes fastest.
Arguments:
- orbitals: bfloat16 [32, 400, 2048], P('walk', None, 'chol'), may hold values from -4 to 4
- intersection_inv: bfloat16 [32, 400, 400], P('walk'), may hold values from -0.18 to 0.18
- interp: bfloat16 [2048, 4096], P(None, 'chol'), may hold values from -0.079549513 to 0.079549513
- occ_interp: bfloat16 [400, 4096], P(None, 'chol'), may hold values from -0.18 to 0.18
- chol_factors: bfloat16 [4096, 8192], P('chol', 'walk'), may hold values from -2 to 2
- fields: float32 [32, 8192], P(None, 'walk'), may hold values from -4 to 4
Outputs:
- new_orbitals: bfloat16 [32, 400, 2048], P('walk', None, 'chol')
- force_bias: float32 [32, 8192], P(None, 'walk')
The draws below stay inside these ranges and needn't reach their ends.
All inputs are finite; a program needn't handle non-finite values.
Results may differ from the reference program's by a relative error of at most 0.017.
Values may be sent and summed in bfloat16 or wider, within the bound.
No kernel may reach another device: no remote copies, remote signals or barrier semaphores. Data moves between devices by JAX's collectives and lax.ppermute only.
A program may use at most 64 MiB of HBM per device.

```python
import jax
import jax.numpy as jnp
from jax import lax

BASIS_SIZE = 2048
ELECTRONS = 400
PTS_DEV = 512
TERMS = 4
POINTS = 4096
VECTORS = 8192
WALKERS = 32
N_CHOL = 8


def bounded_values(key, shape, deviation):
    base = jax.random.truncated_normal(key, -3.5, 3.5, shape, jnp.float32)
    return base * deviation


def draw_orbitals(key, part):
    values = bounded_values(jax.random.fold_in(key, 11), (WALKERS, ELECTRONS, BASIS_SIZE), 1.0)
    return values.astype(jnp.bfloat16)


def draw_intersection_inv(key, part):
    deviation = 1.0 / jnp.sqrt(jnp.float32(ELECTRONS))
    values = bounded_values(jax.random.fold_in(key, 13), (WALKERS, ELECTRONS, ELECTRONS), deviation)
    return values.astype(jnp.bfloat16)


def draw_interp(key, part):
    deviation = 1.0 / jnp.sqrt(jnp.float32(BASIS_SIZE))
    values = bounded_values(jax.random.fold_in(key, 17), (BASIS_SIZE, POINTS), deviation)
    return values.astype(jnp.bfloat16)


def draw_occ_interp(key, part):
    deviation = 1.0 / jnp.sqrt(jnp.float32(ELECTRONS))
    values = bounded_values(jax.random.fold_in(key, 19), (ELECTRONS, POINTS), deviation)
    return values.astype(jnp.bfloat16)


def draw_fields(key, part):
    return bounded_values(jax.random.fold_in(key, 23), (WALKERS, VECTORS), 1.0)


def draw_chol_factors(key, part):
    first_key, second_key = jax.random.split(jax.random.fold_in(key, 7))
    column = jnp.arange(VECTORS).astype(jnp.float32) / VECTORS
    spread = jax.random.uniform(second_key, (VECTORS,), jnp.float32)
    column_scale = 0.2 * 10.0 ** (0.5 * column + 0.5 * spread)
    base = jax.random.truncated_normal(first_key, -4.0, 4.0, (POINTS, VECTORS), jnp.float32)
    normalizer = 0.75 * jnp.sqrt(jnp.float32(BASIS_SIZE) / (jnp.float32(POINTS) * jnp.float32(VECTORS)))
    values = base * column_scale[None, :] * normalizer
    return values.astype(jnp.bfloat16)


def setup_inputs(seed: int = 0) -> dict:
    key_of = jax.random.split(jax.random.key(seed), 7)
    return {
        "orbitals": draw_orbitals(jax.random.fold_in(key_of[6], 71), 0),
        "intersection_inv": draw_intersection_inv(jax.random.fold_in(key_of[6], 71), 0),
        "interp": draw_interp(jax.random.fold_in(key_of[6], 71), 0),
        "occ_interp": draw_occ_interp(jax.random.fold_in(key_of[6], 71), 0),
        "chol_factors": draw_chol_factors(jax.random.fold_in(key_of[6], 71), 0),
        "fields": draw_fields(jax.random.fold_in(key_of[6], 71), 0),
    }


time_root = 2.2


def propagate(orbit, inverse, field_row, interp, occ_interp, chol_factors):
    green = jnp.dot(inverse, orbit, preferred_element_type=jnp.float32).astype(jnp.bfloat16)
    projected = jnp.dot(green, interp, preferred_element_type=jnp.float32)
    weights = jnp.sum(occ_interp.astype(jnp.float32) * projected, axis=0)
    factors = chol_factors.astype(jnp.float32)
    bias = jnp.dot(weights, factors, precision=lax.Precision.HIGHEST)
    coeff = time_root * (field_row - bias)
    scales = jnp.dot(factors, coeff, precision=lax.Precision.HIGHEST)
    total = orbit.astype(jnp.float32)
    term = orbit
    for order in range(1, TERMS + 1):
        product = jnp.dot(term, interp, preferred_element_type=jnp.float32)
        mixed = (product * scales[None, :] / order).astype(jnp.bfloat16)
        summed = jnp.zeros(orbit.shape, jnp.float32)
        for block in range(N_CHOL):
            lower = block * PTS_DEV
            piece = jnp.dot(mixed[:, lower:lower + PTS_DEV], interp[:, lower:lower + PTS_DEV].T, preferred_element_type=jnp.float32)
            rounded = lax.optimization_barrier(piece.astype(jnp.bfloat16))
            summed = summed + rounded.astype(jnp.float32)
        term = summed.astype(jnp.bfloat16)
        total = total + term.astype(jnp.float32)
    return total.astype(jnp.bfloat16), bias


def reference(orbitals, intersection_inv, interp, occ_interp, chol_factors, fields):
    def single(items):
        return propagate(items[0], items[1], items[2], interp, occ_interp, chol_factors)

    new_orbitals, force_bias = lax.map(single, (orbitals, intersection_inv, fields))
    return (new_orbitals, force_bias)
```

```python
import jax
import jax.numpy as jnp
from jax import lax
from jax.experimental import pallas as pl
from jax.experimental.pallas import tpu as pltpu
from jax.sharding import Mesh
from jax.sharding import PartitionSpec as P

TERMS = 4
time_root = 2.2

NZ, NX, NY, NC = 8, 4, 4, 2
ROWS = 400
SLAB = 104
PIECE = 56
TILES = (0, 6, 12, 18, 25, 31, 37, 43, 50)
f32 = jnp.float32
bf16 = jnp.bfloat16


def ring(n, k):
    return [(i, (i + k) % n) for i in range(n)]


PAIRS = [(i, (i + 1) % 8 if i % 2 else (i - 1) % 8) for i in range(8)]


def swap_core(value):
    return lax.ppermute(value, "core", ring(NC, 1))


def to_all(value, axis, length):
    return lax.all_to_all(
        jnp.broadcast_to(value[None], (length, *value.shape)), axis, 0, 0, tiled=True
    )


def one_term(term, scale_refs, interp_refs, out_ref):
    acc = None
    for scale, interp in zip(scale_refs, interp_refs):
        product = jnp.dot(term, interp[...], preferred_element_type=f32)
        mixed = (product * scale).astype(bf16)
        part = lax.dot_general(
            mixed, interp[...], (((1,), (1,)), ((), ())), preferred_element_type=f32
        )
        acc = part if acc is None else acc + part
    out_ref[...] = acc.astype(bf16)


def first_kernel(term_ref, scales_ref, a0, a1, a2, a3, out_ref):
    scales = [scales_ref[b : b + 1, :] for b in range(4)]
    one_term(term_ref[...], scales, (a0, a1, a2, a3), out_ref)


def next_kernel(mine_ref, other_ref, total_ref, scales_ref, a0, a1, a2, a3, out_ref, total_out):
    term = (mine_ref[...].astype(f32) + other_ref[...].astype(f32)).astype(bf16)
    total_out[...] = total_ref[...] + term.astype(f32)
    scales = [scales_ref[b : b + 1, :] for b in range(4)]
    one_term(term, scales, (a0, a1, a2, a3), out_ref)


def vmem(n):
    return [pl.BlockSpec(memory_space=pltpu.VMEM)] * n


def call_first(term, scales, halves):
    return pl.pallas_call(
        first_kernel,
        out_shape=jax.ShapeDtypeStruct((SLAB, 2048), bf16),
        in_specs=vmem(6),
        out_specs=vmem(1)[0],
        name="first_term",
    )(term, scales, *halves)


def call_next(mine, other, total, scales, halves):
    return pl.pallas_call(
        next_kernel,
        out_shape=(
            jax.ShapeDtypeStruct((SLAB, 2048), bf16),
            jax.ShapeDtypeStruct((SLAB, 2048), f32),
        ),
        in_specs=vmem(8),
        out_specs=tuple(vmem(2)),
        name="next_term",
    )(mine, other, total, scales, *halves)


def on_device(orbitals, intersection_inv, interp, occ_interp, chol_factors, fields):
    x = lax.axis_index("x")
    y = lax.axis_index("y")
    c = lax.axis_index("core")
    a_own = interp.reshape(4, 2, 256, 512).transpose(1, 0, 2, 3).reshape(2048, 512)
    a_par = swap_core(a_own)
    occ_par = swap_core(occ_interp)
    chol_par = swap_core(chol_factors)
    cols = to_all(orbitals[0], "y", NY)
    cols = jnp.moveaxis(cols, 0, 1).reshape(ROWS, 1024)
    part = lax.dynamic_slice(a_own, (x * 512, 0), (512, 512))
    part, _ = lax.optimization_barrier((part, cols))
    part = lax.ppermute(part, "y", ring(NY, 2))
    chol_far = lax.ppermute(jnp.concatenate([chol_factors, chol_par], 0), "y", ring(NY, 2))

    green = jnp.dot(intersection_inv[0], cols, preferred_element_type=f32).astype(bf16)
    weights = []
    for a, occ in ((a_own, occ_interp), (a_par, occ_par)):
        rows = lax.dynamic_slice(a, (c * 1024, 0), (1024, 512))
        projected = jnp.dot(green, rows, preferred_element_type=f32)
        weights.append(jnp.sum(occ.astype(f32) * projected, axis=0))
    weights = jnp.concatenate(weights)[None]
    all_weights = to_all(weights, ("z", "x"), NZ * NX).reshape(32, 1024)

    far_own = to_all(part, "x", NX).reshape(2048, 512)
    near = jnp.concatenate([chol_factors, chol_par], 0).astype(f32)
    partial_bias = jnp.dot(all_weights, near, precision=lax.Precision.HIGHEST)
    force_bias = jnp.sum(to_all(partial_bias, ("y", "core"), 8), axis=0)
    coeff = time_root * (fields - force_bias)
    half = jnp.concatenate([near, chol_far.astype(f32)], 0)
    field_part = jnp.dot(coeff, half.T, precision=lax.Precision.HIGHEST)
    arrived = lax.all_to_all(field_part.reshape(32, 4, 512), ("z", "x"), 0, 0, tiled=True)
    scales = jnp.sum(arrived, axis=0)
    far_par = swap_core(far_own)
    halves = (a_own, a_par, far_own, far_par)

    starts = jnp.array([8 * TILES[2 * e] for e in range(4)], jnp.int32)
    mine_at = jnp.where(c == 1, starts[y], starts[(y + 3) % 4])
    other_at = jnp.where(c == 1, starts[(y + 3) % 4], starts[y])
    own_cols = lax.dynamic_slice(cols, (mine_at, 0), (SLAB, 1024))
    par_cols = swap_core(lax.dynamic_slice(cols, (other_at, 0), (SLAB, 1024)))
    term = jnp.where(
        c == 0,
        jnp.concatenate([own_cols, par_cols], 1),
        jnp.concatenate([par_cols, own_cols], 1),
    )
    total = term.astype(f32)
    mine = call_first(term, scales, halves)
    for order in range(2, TERMS + 1):
        other = lax.ppermute(mine, ("y", "core"), PAIRS)
        mine, total = call_next(mine, other, total, scales / order, halves)
    keep_at = jnp.where(c == 1, 0, SLAB - PIECE)
    give_at = jnp.where(c == 1, SLAB - PIECE, 0)
    keep = lax.dynamic_slice(mine, (keep_at, 0), (PIECE, 2048))
    give = lax.dynamic_slice(mine, (give_at, 0), (PIECE, 2048))
    got = lax.ppermute(give, ("y", "core"), PAIRS)
    last = (keep.astype(f32) + got.astype(f32)).astype(bf16).astype(f32)
    total = lax.dynamic_slice(total, (keep_at, 0), (PIECE, 2048))
    rows = (total + last).astype(bf16)
    blocks = rows.reshape(PIECE, 2, 4, 256).transpose(2, 1, 0, 3).reshape(8, PIECE, 256)
    back = lax.all_to_all(blocks, ("y", "core"), 0, 0, tiled=True)
    out = [back[(i + 1) % 8, : 8 * (TILES[i + 1] - TILES[i])] for i in range(8)]
    return jnp.concatenate(out, 0)[None], force_bias


def solution(mesh):
    fine = Mesh(mesh.devices.reshape(NZ, NX, NY, NC), ("z", "x", "y", "core"))
    walk, chol = ("z", "x"), ("y", "core")
    return jax.shard_map(
        on_device,
        mesh=fine,
        in_specs=(
            P(walk, None, chol),
            P(walk, None, None),
            P(None, chol),
            P(None, chol),
            P(chol, walk),
            P(None, walk),
        ),
        out_specs=(P(walk, None, chol), P(None, walk)),
        check_vma=False,
    )
```

```python
import jax
import jax.numpy as jnp
from jax import lax
from jax.experimental import pallas as pl
from jax.experimental.pallas import tpu as pltpu
from jax.sharding import Mesh
from jax.sharding import PartitionSpec as P


TERMS = 4
time_root = 2.2

NZ, NX, NY, NC = 8, 4, 4, 2
ROWS = 400
SLAB = 104
PIECE = 56
TILES = (0, 6, 12, 18, 25, 31, 37, 43, 50)
VMEM_LIMIT = 12 * 2**20
f32 = jnp.float32
bf16 = jnp.bfloat16


def ring(n, k):
    return [(i, (i + k) % n) for i in range(n)]


PAIRS = [(i, (i + 1) % 8 if i % 2 else (i - 1) % 8) for i in range(8)]


def swap_core(value):
    return lax.ppermute(value, "core", ring(NC, 1))


def to_all(value, axis, length):
    return lax.all_to_all(
        jnp.broadcast_to(value[None], (length, *value.shape)), axis, 0, 0, tiled=True
    )


def spec(space):
    return pl.BlockSpec(memory_space=space)


PARAMS = pltpu.CompilerParams(vmem_limit_bytes=VMEM_LIMIT)


def edge_of(y, c):
    return jnp.where(c == 1, y, (y + 3) % 4)


def head_kernel(inv, o0, o1, o2, o3, a_own, a_par, occ_own, occ_par, weights_ref):
    y = lax.axis_index("y")
    c = lax.axis_index("core")
    sums = [None, None]
    for j, o in enumerate((o0, o1, o2, o3)):
        green = jnp.dot(inv[...], o[...], preferred_element_type=f32).astype(bf16)
        at = pl.multiple_of(((y + j) % 4) * 512 + c * 256, 256)
        for k, a in enumerate((a_own, a_par)):
            part = jnp.dot(green, a[pl.ds(at, 256), :], preferred_element_type=f32)
            sums[k] = part if sums[k] is None else sums[k] + part
    for k, occ in enumerate((occ_own, occ_par)):
        weights = jnp.sum(occ[...].astype(f32) * sums[k], axis=0, keepdims=True)
        weights_ref[:, :, 512 * k : 512 * k + 512] = jnp.broadcast_to(weights, (32, 1, 512))


def call_head(inv, cols, a_own, a_par, occ_own, occ_par):
    return pl.pallas_call(
        head_kernel,
        out_shape=jax.ShapeDtypeStruct((32, 1, 1024), f32),
        in_specs=[spec(pltpu.VMEM)] * 9,
        out_specs=spec(pltpu.VMEM),
        compiler_params=pltpu.CompilerParams(vmem_limit_bytes=24 * 2**20),
        name="head",
    )(inv, *cols, a_own, a_par, occ_own, occ_par)


def slab_kernel(o0, o1, o2, o3, mine_ref, other_ref, sems):
    y = lax.axis_index("y")
    c = lax.axis_index("core")
    copies = []
    for k, out in enumerate((mine_ref, other_ref)):
        edge = edge_of(y, c if k == 0 else 1 - c)
        row = edge * 96 + jnp.where(edge >= 2, 8, 0)
        for j, o in enumerate((o0, o1, o2, o3)):
            copy = pltpu.make_async_copy(
                o.at[pl.ds(pl.multiple_of(row, 8), SLAB), :],
                out.at[:, pl.ds(pl.multiple_of(((y + j) % 4) * 256, 256), 256)],
                sems.at[4 * k + j],
            )
            copy.start()
            copies.append(copy)
    for copy in copies:
        copy.wait()


def call_slabs(cols):
    return pl.pallas_call(
        slab_kernel,
        out_shape=(jax.ShapeDtypeStruct((SLAB, 1024), bf16),) * 2,
        in_specs=[spec(pl.ANY)] * 4,
        out_specs=(spec(pl.ANY),) * 2,
        scratch_shapes=[pltpu.SemaphoreType.DMA((8,))],
        compiler_params=PARAMS,
        name="slabs",
    )(*cols)


def join_kernel(own, par, term_ref):
    c = lax.axis_index("core")

    def put(first, second):
        for y in range(4):
            cols = slice(256 * y, 256 * y + 256)
            term_ref[:, 512 * y : 512 * y + 256] = first[:, cols]
            term_ref[:, 512 * y + 256 : 512 * y + 512] = second[:, cols]

    pl.when(c == 0)(lambda: put(own, par))
    pl.when(c == 1)(lambda: put(par, own))


def call_join(own, par):
    return pl.pallas_call(
        join_kernel,
        out_shape=jax.ShapeDtypeStruct((SLAB, 2048), bf16),
        in_specs=[spec(pltpu.VMEM)] * 2,
        out_specs=spec(pltpu.VMEM),
        compiler_params=PARAMS,
        name="join",
    )(own, par)


def load_kernel(a0, a1, f0, f1, out_ref, sems):
    x = lax.axis_index("x")
    copies = [pltpu.make_async_copy(a, out_ref.at[b], sems.at[b]) for b, a in enumerate((a0, a1))]
    for b, f in enumerate((f0, f1)):
        for j in range(NX):
            at = pl.multiple_of(((x + j) % NX) * 512, 512)
            copies.append(
                pltpu.make_async_copy(
                    f.at[pl.ds(512 * j, 512), :],
                    out_ref.at[2 + b, pl.ds(at, 512), :],
                    sems.at[2 + NX * b + j],
                )
            )
    for copy in copies:
        copy.start()
    for copy in copies:
        copy.wait()


def call_load(halves):
    out = pl.pallas_call(
        load_kernel,
        out_shape=pltpu.VMEM((4, 2048, 512), bf16),
        in_specs=[spec(pl.ANY)] * 4,
        out_specs=spec(pltpu.VMEM),
        scratch_shapes=[pltpu.SemaphoreType.DMA((2 + 2 * NX,))],
        compiler_params=PARAMS,
        name="load_halves",
    )(*halves)
    return pltpu.with_memory_space_constraint(out, pltpu.VMEM)


def one_term(term, scales_ref, order, interp_ref):
    acc = None
    for b in range(4):
        interp = interp_ref[b]
        product = jnp.dot(term, interp, preferred_element_type=f32)
        mixed = (product * (scales_ref[b : b + 1, :] / order)).astype(bf16)
        part = lax.dot_general(
            mixed, interp, (((1,), (1,)), ((), ())), preferred_element_type=f32
        )
        acc = part if acc is None else acc + part
    return acc


def first_kernel(term_ref, scales_ref, interp_ref, out_ref):
    out_ref[...] = one_term(term_ref[...], scales_ref, 1, interp_ref).astype(bf16)


def next_kernel(order, mine_ref, other_ref, total_ref, scales_ref, interp_ref, out_ref, total_out):
    term = (mine_ref[...].astype(f32) + other_ref[...].astype(f32)).astype(bf16)
    total_out[...] = total_ref[...].astype(f32) + term.astype(f32)
    out_ref[...] = one_term(term, scales_ref, order, interp_ref).astype(bf16)


def last_kernel(mine_ref, other_ref, total_ref, scales_ref, interp_ref, out_ref):
    c = lax.axis_index("core")
    term = (mine_ref[...].astype(f32) + other_ref[...].astype(f32)).astype(bf16)
    total = total_ref[...] + term.astype(f32)
    acc = one_term(term, scales_ref, TERMS, interp_ref)
    low, high = slice(0, PIECE), slice(SLAB - PIECE, SLAB)

    def put(keep, give):
        kept = (acc[keep] + total[keep]).astype(bf16)
        given = acc[give].astype(bf16)
        for b in range(8):
            out_ref[b, :PIECE, :] = kept[:, 256 * b : 256 * b + 256]
            out_ref[b, PIECE:, :] = given[:, 256 * b : 256 * b + 256]

    pl.when(c == 1)(lambda: put(low, high))
    pl.when(c == 0)(lambda: put(high, low))


def call_term(kernel, out_shape, *args):
    many = isinstance(out_shape, tuple)
    return pl.pallas_call(
        kernel,
        out_shape=out_shape,
        in_specs=[spec(pltpu.VMEM)] * len(args),
        out_specs=(spec(pltpu.VMEM),) * len(out_shape) if many else spec(pltpu.VMEM),
        compiler_params=PARAMS,
        name="term",
    )(*args)


def end_kernel(back_ref, out_ref):
    for i in range(8):
        start = 8 * TILES[i]
        n = 8 * (TILES[i + 1] - TILES[i])
        owner, partner = (i + 1) % 8, (i + 2) % 8 if i % 2 == 0 else i
        kept = back_ref[owner, :n, :].astype(f32)
        given = back_ref[partner, PIECE : PIECE + n, :].astype(f32)
        out_ref[0, start : start + n, :] = (kept + given).astype(bf16)


def call_end(back):
    return pl.pallas_call(
        end_kernel,
        out_shape=jax.ShapeDtypeStruct((1, ROWS, 256), bf16),
        in_specs=[spec(pltpu.VMEM)],
        out_specs=spec(pltpu.VMEM),
        compiler_params=PARAMS,
        name="end",
    )(back)


def on_device(orbitals, intersection_inv, interp, occ_interp, chol_factors, fields):
    x = lax.axis_index("x")
    cols = [orbitals[0]]
    for j in (1, 2, 3):
        cols.append(lax.ppermute(orbitals[0], "y", ring(NY, -j)))
    a_par = swap_core(interp)
    occ_par = swap_core(occ_interp)
    chol_par = swap_core(chol_factors)
    near = jnp.concatenate([chol_factors, chol_par], 0)
    part = lax.dynamic_slice(interp, (x * 512, 0), (512, 512))
    part = lax.ppermute(part, "y", ring(NY, 2))
    chol_far = lax.ppermute(near, "y", ring(NY, 2))

    weights = call_head(intersection_inv[0], cols, interp, a_par, occ_interp, occ_par)
    mine, other = call_slabs(cols)
    term = call_join(mine, swap_core(other))
    all_weights = lax.all_to_all(weights, ("z", "x"), 0, 0, tiled=True).reshape(32, 1024)

    parts = [part]
    for j in (1, 2, 3):
        parts.append(lax.ppermute(part, "x", ring(NX, -j)))
    far_own = jnp.concatenate(parts, 0)
    partial_bias = jnp.dot(all_weights, near.astype(f32), precision=lax.Precision.HIGHEST)
    force_bias = jnp.sum(to_all(partial_bias, ("y", "core"), 8), axis=0)
    coeff = time_root * (fields - force_bias)
    half = jnp.concatenate([near, chol_far], 0).astype(f32)
    field_part = jnp.dot(coeff, half.T, precision=lax.Precision.HIGHEST)
    arrived = lax.all_to_all(
        field_part.astype(bf16).reshape(32, 4, 512), ("z", "x"), 0, 0, tiled=True
    )
    scales = jnp.sum(arrived.astype(f32), axis=0)
    far_par = swap_core(far_own)
    halves = call_load((interp, a_par, far_own, far_par))

    part_shape = jax.ShapeDtypeStruct((SLAB, 2048), bf16)
    total_shape = jax.ShapeDtypeStruct((SLAB, 2048), f32)
    total = term
    mine = call_term(first_kernel, part_shape, term, scales, halves)
    for order in range(2, TERMS):
        other = lax.ppermute(mine, ("y", "core"), PAIRS)
        mine, total = call_term(
            lambda *refs, order=order: next_kernel(order, *refs),
            (part_shape, total_shape),
            *(mine, other, total, scales, halves),
        )
    other = lax.ppermute(mine, ("y", "core"), PAIRS)
    blocks = call_term(
        last_kernel,
        jax.ShapeDtypeStruct((8, 2 * PIECE, 256), bf16),
        *(mine, other, total, scales, halves),
    )
    back = lax.all_to_all(blocks, ("y", "core"), 0, 0, tiled=True)
    return call_end(back), force_bias


def solution(mesh):
    fine = Mesh(mesh.devices.reshape(NZ, NX, NY, NC), ("z", "x", "y", "core"))
    walk, chol = ("z", "x"), ("y", "core")
    return jax.shard_map(
        on_device,
        mesh=fine,
        in_specs=(
            P(walk, None, chol),
            P(walk, None, None),
            P(None, chol),
            P(None, chol),
            P(chol, walk),
            P(None, walk),
        ),
        out_specs=(P(walk, None, chol), P(None, walk)),
        check_vma=False,
    )
```

```python
import jax
import jax.numpy as jnp
from jax import lax
from jax.experimental import pallas as pl
from jax.experimental.pallas import tpu as pltpu
from jax.sharding import Mesh
from jax.sharding import PartitionSpec as P


TERMS = 4
time_root = 2.2

NZ, NX, NY, NC = 8, 4, 4, 2
ROWS = 400
SLAB = 104
PIECE = 56
TILES = (0, 6, 12, 18, 25, 31, 37, 43, 50)
VMEM_LIMIT = 12 * 2**20
f32 = jnp.float32
bf16 = jnp.bfloat16


def ring(n, k):
    return [(i, (i + k) % n) for i in range(n)]


PAIRS = [(i, (i + 1) % 8 if i % 2 else (i - 1) % 8) for i in range(8)]


def swap_core(value):
    return lax.ppermute(value, "core", ring(NC, 1))


def to_all(value, axis, length):
    return lax.all_to_all(
        jnp.broadcast_to(value[None], (length, *value.shape)), axis, 0, 0, tiled=True
    )


def spec(space):
    return pl.BlockSpec(memory_space=space)


def in_hbm(*values):
    return [pltpu.with_memory_space_constraint(v, pltpu.HBM) for v in values]


PARAMS = pltpu.CompilerParams(vmem_limit_bytes=VMEM_LIMIT)


def edge_of(y, c):
    return jnp.where(c == 1, y, (y + 3) % 4)


def start_kernel(interp, inv, orb, occ, part, rows_out, inv_out, orb_out, occ_out, sems):
    x = lax.axis_index("x")
    c = lax.axis_index("core")
    at = pl.multiple_of(x * 512, 512)
    copies = [pltpu.make_async_copy(interp.at[pl.ds(at, 512), :], part, sems.at[0])]
    for y in range(NY):
        at = pl.multiple_of(y * 512 + c * 256, 256)
        rows = interp.at[pl.ds(at, 256), :]
        copies.append(
            pltpu.make_async_copy(rows, rows_out.at[pl.ds(256 * y, 256), :], sems.at[1 + y])
        )
    for k, (a, b) in enumerate(((inv, inv_out), (orb, orb_out), (occ, occ_out))):
        copies.append(pltpu.make_async_copy(a, b, sems.at[5 + k]))
    for copy in copies:
        copy.start()
    for copy in copies:
        copy.wait()


def call_start(interp, inv, orb, occ):
    part, *rest = pl.pallas_call(
        start_kernel,
        out_shape=(
            jax.ShapeDtypeStruct((512, 512), bf16),
            pltpu.VMEM((1024, 512), bf16),
            pltpu.VMEM((ROWS, ROWS), bf16),
            pltpu.VMEM((ROWS, 256), bf16),
            pltpu.VMEM((ROWS, 512), bf16),
        ),
        in_specs=[spec(pltpu.HBM)] * 4,
        out_specs=(spec(pltpu.HBM),) + (spec(pltpu.VMEM),) * 4,
        scratch_shapes=[pltpu.SemaphoreType.DMA((8,))],
        compiler_params=PARAMS,
        name="start",
    )(*in_hbm(interp, inv, orb, occ))
    return part, *[pltpu.with_memory_space_constraint(r, pltpu.VMEM) for r in rest]


def head_kernel(inv, o0, o1, o2, o3, rows_own, a_par, occ_own, occ_par, weights_ref):
    y = lax.axis_index("y")
    c = lax.axis_index("core")
    sums = [None, None]
    for j, o in enumerate((o0, o1, o2, o3)):
        green = jnp.dot(inv[...], o[...], preferred_element_type=f32).astype(bf16)
        of = (y + j) % NY
        own = rows_own[pl.ds(pl.multiple_of(of * 256, 256), 256), :]
        par = a_par[pl.ds(pl.multiple_of(of * 512 + c * 256, 256), 256), :]
        for k, a in enumerate((own, par)):
            part = jnp.dot(green, a, preferred_element_type=f32)
            sums[k] = part if sums[k] is None else sums[k] + part
    for k, occ in enumerate((occ_own, occ_par)):
        weights = jnp.sum(occ[...].astype(f32) * sums[k], axis=0, keepdims=True)
        weights_ref[:, :, 512 * k : 512 * k + 512] = jnp.broadcast_to(weights, (32, 1, 512))


def call_head(inv, cols, rows_own, a_par, occ_own, occ_par):
    return pl.pallas_call(
        head_kernel,
        out_shape=jax.ShapeDtypeStruct((32, 1, 1024), f32),
        in_specs=[spec(pltpu.VMEM)] * 9,
        out_specs=spec(pltpu.VMEM),
        compiler_params=pltpu.CompilerParams(vmem_limit_bytes=24 * 2**20),
        name="head",
    )(inv, *cols, rows_own, a_par, occ_own, occ_par)


def field_kernel(bias_ref, fields_ref, c0, c1, c2, c3, force_ref, out_ref):
    bias = bias_ref[0]
    for k in range(1, 8):
        bias = bias + bias_ref[k]
    force_ref[...] = bias
    coeff = time_root * (fields_ref[...] - bias)
    parts = [
        lax.dot_general(
            coeff,
            c[...].astype(f32),
            (((1,), (1,)), ((), ())),
            precision=lax.Precision.HIGHEST,
            preferred_element_type=f32,
        )
        for c in (c0, c1, c2, c3)
    ]
    out_ref[...] = jnp.concatenate(parts, 1).reshape(32, 4, 512).astype(bf16)


def call_field(biases, fields, chols):
    return pl.pallas_call(
        field_kernel,
        out_shape=(
            jax.ShapeDtypeStruct((32, 256), f32),
            jax.ShapeDtypeStruct((32, 4, 512), bf16),
        ),
        in_specs=[spec(pltpu.VMEM)] * 6,
        out_specs=(spec(pltpu.VMEM),) * 2,
        compiler_params=PARAMS,
        name="field",
    )(biases, fields, *chols)


def slab_kernel(o0, o1, o2, o3, mine_ref, other_ref, sems):
    y = lax.axis_index("y")
    c = lax.axis_index("core")
    copies = []
    for k, out in enumerate((mine_ref, other_ref)):
        edge = edge_of(y, c if k == 0 else 1 - c)
        row = edge * 96 + jnp.where(edge >= 2, 8, 0)
        for j, o in enumerate((o0, o1, o2, o3)):
            copy = pltpu.make_async_copy(
                o.at[pl.ds(pl.multiple_of(row, 8), SLAB), :],
                out.at[:, pl.ds(pl.multiple_of(((y + j) % 4) * 256, 256), 256)],
                sems.at[4 * k + j],
            )
            copy.start()
            copies.append(copy)
    for copy in copies:
        copy.wait()


def call_slabs(cols):
    return pl.pallas_call(
        slab_kernel,
        out_shape=(jax.ShapeDtypeStruct((SLAB, 1024), bf16),) * 2,
        in_specs=[spec(pl.ANY)] * 4,
        out_specs=(spec(pl.ANY),) * 2,
        scratch_shapes=[pltpu.SemaphoreType.DMA((8,))],
        compiler_params=PARAMS,
        name="slabs",
    )(*cols)


def join_kernel(own, par, term_ref):
    c = lax.axis_index("core")

    def put(first, second):
        for y in range(4):
            cols = slice(256 * y, 256 * y + 256)
            term_ref[:, 512 * y : 512 * y + 256] = first[:, cols]
            term_ref[:, 512 * y + 256 : 512 * y + 512] = second[:, cols]

    pl.when(c == 0)(lambda: put(own, par))
    pl.when(c == 1)(lambda: put(par, own))


def call_join(own, par):
    return pl.pallas_call(
        join_kernel,
        out_shape=jax.ShapeDtypeStruct((SLAB, 2048), bf16),
        in_specs=[spec(pltpu.VMEM)] * 2,
        out_specs=spec(pltpu.VMEM),
        compiler_params=PARAMS,
        name="join",
    )(own, par)


def one_term(term, scales_ref, order, interp_ref, wait=lambda b: None):
    acc = None
    for b in range(4):
        wait(b)
        interp = interp_ref[b]
        product = jnp.dot(term, interp, preferred_element_type=f32)
        mixed = (product * (scales_ref[b : b + 1, :] / order)).astype(bf16)
        part = lax.dot_general(
            mixed, interp, (((1,), (1,)), ((), ())), preferred_element_type=f32
        )
        acc = part if acc is None else acc + part
    return acc


def first_kernel(term_ref, arrived_ref, *refs):
    near, far, (out_ref, scales_ref, interp_ref, sems) = refs[:2], (refs[2:6], refs[6:10]), refs[10:]
    x = lax.axis_index("x")
    copies = [
        [pltpu.make_async_copy(a, interp_ref.at[b], sems.at[b])] for b, a in enumerate(near)
    ]
    for b in range(2):
        copies.append([])
        for j in range(NX):
            at = pl.multiple_of(((x + j) % NX) * 512, 512)
            copies[-1].append(
                pltpu.make_async_copy(
                    far[b][j], interp_ref.at[2 + b, pl.ds(at, 512), :], sems.at[2 + NX * b + j]
                )
            )
    for copy in sum(copies, []):
        copy.start()
    scales_ref[...] = jnp.sum(arrived_ref[...].astype(f32), axis=0)

    def wait(b):
        for copy in copies[b]:
            copy.wait()

    out_ref[...] = one_term(term_ref[...], scales_ref, 1, interp_ref, wait).astype(bf16)


def call_first(term, arrived, parts):
    mine, scales, halves = pl.pallas_call(
        first_kernel,
        out_shape=(
            jax.ShapeDtypeStruct((SLAB, 2048), bf16),
            jax.ShapeDtypeStruct((4, 512), f32),
            pltpu.VMEM((4, 2048, 512), bf16),
        ),
        in_specs=[spec(pltpu.VMEM)] * 2 + [spec(pltpu.HBM)] * 10,
        out_specs=(spec(pltpu.VMEM),) * 3,
        scratch_shapes=[pltpu.SemaphoreType.DMA((2 + 2 * NX,))],
        compiler_params=PARAMS,
        name="first",
    )(term, arrived, *in_hbm(*parts))
    return mine, scales, pltpu.with_memory_space_constraint(halves, pltpu.VMEM)


def next_kernel(order, mine_ref, other_ref, total_ref, scales_ref, interp_ref, out_ref, total_out):
    term = (mine_ref[...].astype(f32) + other_ref[...].astype(f32)).astype(bf16)
    total_out[...] = total_ref[...].astype(f32) + term.astype(f32)
    out_ref[...] = one_term(term, scales_ref, order, interp_ref).astype(bf16)


def last_kernel(mine_ref, other_ref, total_ref, scales_ref, interp_ref, out_ref):
    c = lax.axis_index("core")
    term = (mine_ref[...].astype(f32) + other_ref[...].astype(f32)).astype(bf16)
    total = total_ref[...] + term.astype(f32)
    acc = one_term(term, scales_ref, TERMS, interp_ref)
    low, high = slice(0, PIECE), slice(SLAB - PIECE, SLAB)

    def put(keep, give):
        kept = (acc[keep] + total[keep]).astype(bf16)
        given = acc[give].astype(bf16)
        for b in range(8):
            out_ref[b, :PIECE, :] = kept[:, 256 * b : 256 * b + 256]
            out_ref[b, PIECE:, :] = given[:, 256 * b : 256 * b + 256]

    pl.when(c == 1)(lambda: put(low, high))
    pl.when(c == 0)(lambda: put(high, low))


def call_term(kernel, out_shape, *args):
    many = isinstance(out_shape, tuple)
    return pl.pallas_call(
        kernel,
        out_shape=out_shape,
        in_specs=[spec(pltpu.VMEM)] * len(args),
        out_specs=(spec(pltpu.VMEM),) * len(out_shape) if many else spec(pltpu.VMEM),
        compiler_params=PARAMS,
        name="term",
    )(*args)


def end_kernel(back_ref, out_ref):
    for i in range(8):
        start = 8 * TILES[i]
        n = 8 * (TILES[i + 1] - TILES[i])
        owner, partner = (i + 1) % 8, (i + 2) % 8 if i % 2 == 0 else i
        kept = back_ref[owner, :n, :].astype(f32)
        given = back_ref[partner, PIECE : PIECE + n, :].astype(f32)
        out_ref[0, start : start + n, :] = (kept + given).astype(bf16)


def call_end(back):
    return pl.pallas_call(
        end_kernel,
        out_shape=jax.ShapeDtypeStruct((1, ROWS, 256), bf16),
        in_specs=[spec(pltpu.VMEM)],
        out_specs=spec(pltpu.VMEM),
        compiler_params=PARAMS,
        name="end",
    )(back)


def on_device(orbitals, intersection_inv, interp, occ_interp, chol_factors, fields):
    orb = orbitals[0]
    part, rows, inv, orb_v, occ = call_start(interp, intersection_inv[0], orb, occ_interp)
    others = [lax.ppermute(orb, "y", ring(NY, -j)) for j in (1, 2, 3)]
    a_par = swap_core(interp)
    occ_par = swap_core(occ_interp)
    chol_par = swap_core(chol_factors)
    part, *others = lax.optimization_barrier((part, *others))
    part = lax.ppermute(part, "y", ring(NY, 2))
    chol_far = lax.ppermute(chol_factors, "y", ring(NY, 2))
    chol_far_par = swap_core(chol_far)

    weights = call_head(inv, [orb_v, *others], rows, a_par, occ, occ_par)
    mine, other = call_slabs([orb, *others])
    term = call_join(mine, swap_core(other))
    all_weights = lax.all_to_all(weights, ("z", "x"), 0, 0, tiled=True).reshape(32, 1024)

    far = [part]
    for j in (1, 2, 3):
        far.append(lax.ppermute(part, "x", ring(NX, -j)))
    far_par = []
    for j in range(4):
        far_par.append(swap_core(far[j]))
    near = jnp.concatenate([chol_factors, chol_par], 0).astype(f32)
    partial_bias = jnp.dot(all_weights, near, precision=lax.Precision.HIGHEST)
    biases = to_all(partial_bias, ("y", "core"), 8)
    force_bias, field_part = call_field(
        biases, fields, (chol_factors, chol_par, chol_far, chol_far_par)
    )
    arrived = lax.all_to_all(field_part, ("z", "x"), 0, 0, tiled=True)

    part_shape = jax.ShapeDtypeStruct((SLAB, 2048), bf16)
    total_shape = jax.ShapeDtypeStruct((SLAB, 2048), f32)
    total = term
    mine, scales, halves = call_first(term, arrived, (interp, a_par, *far, *far_par))
    for order in range(2, TERMS):
        other = lax.ppermute(mine, ("y", "core"), PAIRS)
        mine, total = call_term(
            lambda *refs, order=order: next_kernel(order, *refs),
            (part_shape, total_shape),
            *(mine, other, total, scales, halves),
        )
    other = lax.ppermute(mine, ("y", "core"), PAIRS)
    blocks = call_term(
        last_kernel,
        jax.ShapeDtypeStruct((8, 2 * PIECE, 256), bf16),
        *(mine, other, total, scales, halves),
    )
    back = lax.all_to_all(blocks, ("y", "core"), 0, 0, tiled=True)
    return call_end(back), force_bias


def solution(mesh):
    fine = Mesh(mesh.devices.reshape(NZ, NX, NY, NC), ("z", "x", "y", "core"))
    walk, chol = ("z", "x"), ("y", "core")
    return jax.shard_map(
        on_device,
        mesh=fine,
        in_specs=(
            P(walk, None, chol),
            P(walk, None, None),
            P(None, chol),
            P(None, chol),
            P(chol, walk),
            P(None, walk),
        ),
        out_specs=(P(walk, None, chol), P(None, walk)),
        check_vma=False,
    )
```

```python
import jax
import jax.numpy as jnp
from jax import lax
from jax.experimental import pallas as pl
from jax.experimental.pallas import tpu as pltpu
from jax.sharding import Mesh
from jax.sharding import PartitionSpec as P


TERMS = 4
time_root = 2.2

NZ, NX, NY, NC = 8, 4, 4, 2
ROWS = 400
SLAB = 104
HALF = 1024
PIECE = 56
TILES = (0, 6, 12, 18, 25, 31, 37, 43, 50)
VMEM_LIMIT = 12 * 2**20
f32 = jnp.float32
bf16 = jnp.bfloat16


def ring(n, k):
    return [(i, (i + k) % n) for i in range(n)]


PAIRS = [(i, (i + 1) % 8 if i % 2 else (i - 1) % 8) for i in range(8)]


def swap_core(value):
    return lax.ppermute(value, "core", ring(NC, 1))


def to_all(value, axis, length):
    return lax.all_to_all(
        jnp.broadcast_to(value[None], (length, *value.shape)), axis, 0, 0, tiled=True
    )


def spec(space):
    return pl.BlockSpec(memory_space=space)


def in_hbm(*values):
    return [pltpu.with_memory_space_constraint(v, pltpu.HBM) for v in values]


PARAMS = pltpu.CompilerParams(vmem_limit_bytes=VMEM_LIMIT)


def edge_of(y, c):
    return jnp.where(c == 1, y, (y + 3) % 4)


def start_kernel(interp, inv, orb, occ, part, rows_out, inv_out, orb_out, occ_out, sems):
    x = lax.axis_index("x")
    c = lax.axis_index("core")
    at = pl.multiple_of(x * 512, 512)
    copies = [pltpu.make_async_copy(interp.at[pl.ds(at, 512), :], part, sems.at[0])]
    for y in range(NY):
        at = pl.multiple_of(y * 512 + c * 256, 256)
        rows = interp.at[pl.ds(at, 256), :]
        copies.append(
            pltpu.make_async_copy(rows, rows_out.at[pl.ds(256 * y, 256), :], sems.at[1 + y])
        )
    for k, (a, b) in enumerate(((inv, inv_out), (orb, orb_out), (occ, occ_out))):
        copies.append(pltpu.make_async_copy(a, b, sems.at[5 + k]))
    for copy in copies:
        copy.start()
    for copy in copies:
        copy.wait()


def call_start(interp, inv, orb, occ):
    part, *rest = pl.pallas_call(
        start_kernel,
        out_shape=(
            pltpu.VMEM((512, 512), bf16),
            pltpu.VMEM((1024, 512), bf16),
            pltpu.VMEM((ROWS, ROWS), bf16),
            pltpu.VMEM((ROWS, 256), bf16),
            pltpu.VMEM((ROWS, 512), bf16),
        ),
        in_specs=[spec(pltpu.HBM)] * 4,
        out_specs=(spec(pltpu.VMEM),) * 5,
        scratch_shapes=[pltpu.SemaphoreType.DMA((8,))],
        compiler_params=PARAMS,
        name="start",
    )(*in_hbm(interp, inv, orb, occ))
    return part, *[pltpu.with_memory_space_constraint(r, pltpu.VMEM) for r in rest]


def head_kernel(inv, o0, o1, o2, o3, rows_own, a_par, occ_own, occ_par, weights_ref):
    y = lax.axis_index("y")
    c = lax.axis_index("core")
    sums = [None, None]
    for j, o in enumerate((o0, o1, o2, o3)):
        green = jnp.dot(inv[...], o[...], preferred_element_type=f32).astype(bf16)
        of = (y + j) % NY
        own = rows_own[pl.ds(pl.multiple_of(of * 256, 256), 256), :]
        par = a_par[pl.ds(pl.multiple_of(of * 512 + c * 256, 256), 256), :]
        for k, a in enumerate((own, par)):
            part = jnp.dot(green, a, preferred_element_type=f32)
            sums[k] = part if sums[k] is None else sums[k] + part
    for k, occ in enumerate((occ_own, occ_par)):
        weights = jnp.sum(occ[...].astype(f32) * sums[k], axis=0, keepdims=True)
        weights_ref[:, :, 512 * k : 512 * k + 512] = jnp.broadcast_to(weights, (32, 1, 512))


def call_head(inv, cols, rows_own, a_par, occ_own, occ_par):
    return pl.pallas_call(
        head_kernel,
        out_shape=jax.ShapeDtypeStruct((32, 1, 1024), f32),
        in_specs=[spec(pltpu.VMEM)] * 9,
        out_specs=spec(pltpu.VMEM),
        compiler_params=pltpu.CompilerParams(vmem_limit_bytes=24 * 2**20),
        name="head",
    )(inv, *cols, rows_own, a_par, occ_own, occ_par)


def field_kernel(bias_ref, fields_ref, c0, c1, c2, c3, force_ref, out_ref):
    bias = bias_ref[0]
    for k in range(1, 8):
        bias = bias + bias_ref[k]
    force_ref[...] = bias
    coeff = time_root * (fields_ref[...] - bias)
    parts = [
        lax.dot_general(
            coeff,
            c[...].astype(f32),
            (((1,), (1,)), ((), ())),
            precision=lax.Precision.HIGHEST,
            preferred_element_type=f32,
        )
        for c in (c0, c1, c2, c3)
    ]
    out_ref[...] = jnp.concatenate(parts, 1).reshape(32, 4, 512).astype(bf16)


def call_field(biases, fields, chols):
    return pl.pallas_call(
        field_kernel,
        out_shape=(
            jax.ShapeDtypeStruct((32, 256), f32),
            jax.ShapeDtypeStruct((32, 4, 512), bf16),
        ),
        in_specs=[spec(pltpu.VMEM)] * 6,
        out_specs=(spec(pltpu.VMEM),) * 2,
        compiler_params=PARAMS,
        name="field",
    )(biases, fields, *chols)


def slab_kernel(o0, o1, o2, o3, mine_ref, other_ref, sems):
    y = lax.axis_index("y")
    c = lax.axis_index("core")
    copies = []
    for k, out in enumerate((mine_ref, other_ref)):
        edge = edge_of(y, c if k == 0 else 1 - c)
        row = edge * 96 + jnp.where(edge >= 2, 8, 0)
        for j, o in enumerate((o0, o1, o2, o3)):
            copy = pltpu.make_async_copy(
                o.at[pl.ds(pl.multiple_of(row, 8), SLAB), :],
                out.at[:, pl.ds(pl.multiple_of(((y + j) % 4) * 256, 256), 256)],
                sems.at[4 * k + j],
            )
            copy.start()
            copies.append(copy)
    for copy in copies:
        copy.wait()


def call_slabs(cols):
    return pl.pallas_call(
        slab_kernel,
        out_shape=(jax.ShapeDtypeStruct((SLAB, 1024), bf16),) * 2,
        in_specs=[spec(pl.ANY)] * 4,
        out_specs=(spec(pl.ANY),) * 2,
        scratch_shapes=[pltpu.SemaphoreType.DMA((8,))],
        compiler_params=PARAMS,
        name="slabs",
    )(*cols)


def join_kernel(own, par, *outs):
    c = lax.axis_index("core")

    def put(first, second):
        for y in range(4):
            cols, out, at = slice(256 * y, 256 * y + 256), outs[y // 2], 512 * (y % 2)
            out[:, at : at + 256] = first[:, cols]
            out[:, at + 256 : at + 512] = second[:, cols]

    pl.when(c == 0)(lambda: put(own, par))
    pl.when(c == 1)(lambda: put(par, own))


def call_join(own, par):
    return pl.pallas_call(
        join_kernel,
        out_shape=(jax.ShapeDtypeStruct((SLAB, HALF), bf16),) * 2,
        in_specs=[spec(pltpu.VMEM)] * 2,
        out_specs=(spec(pltpu.VMEM),) * 2,
        compiler_params=PARAMS,
        name="join",
    )(own, par)


def times(term, interp_ref, b, h):
    rows = interp_ref[b, HALF * h : HALF * h + HALF, :]
    return jnp.dot(term, rows, preferred_element_type=f32)


def back(mixed, interp_ref, h):
    acc = None
    for b in range(4):
        rows = interp_ref[b, HALF * h : HALF * h + HALF, :]
        part = lax.dot_general(mixed[b], rows, (((1,), (1,)), ((), ())), preferred_element_type=f32)
        acc = part if acc is None else acc + part
    return acc


def mix(product, scales_ref, b, order):
    return (product * (scales_ref[b : b + 1, :] / order)).astype(bf16)


def added(mine_ref, other_ref):
    return (mine_ref[...].astype(f32) + other_ref[...].astype(f32)).astype(bf16)


def first_kernel(term_0, term_1, arrived_ref, *refs):
    near, far = refs[:2], (refs[2:6], refs[6:10])
    mixed_ref, out_ref, scales_ref, interp_ref, sems = refs[10:]
    x = lax.axis_index("x")
    copies = [
        [pltpu.make_async_copy(a, interp_ref.at[b], sems.at[b])] for b, a in enumerate(near)
    ]
    for b in range(2):
        copies.append([])
        for j in range(NX):
            at = pl.multiple_of(((x + j) % NX) * 512, 512)
            copies[-1].append(
                pltpu.make_async_copy(
                    far[b][j], interp_ref.at[2 + b, pl.ds(at, 512), :], sems.at[2 + NX * b + j]
                )
            )
    for copy in sum(copies, []):
        copy.start()
    scales_ref[...] = jnp.sum(arrived_ref[...].astype(f32), axis=0)
    mixed = []
    for b in range(4):
        for copy in copies[b]:
            copy.wait()
        product = times(term_0[...], interp_ref, b, 0) + times(term_1[...], interp_ref, b, 1)
        mixed.append(mix(product, scales_ref, b, 1))
        mixed_ref[b] = mixed[b]
    out_ref[...] = back(mixed, interp_ref, 0).astype(bf16)


def call_first(terms, arrived, parts):
    mixed, mine, scales, halves = pl.pallas_call(
        first_kernel,
        out_shape=(
            jax.ShapeDtypeStruct((4, SLAB, 512), bf16),
            jax.ShapeDtypeStruct((SLAB, HALF), bf16),
            jax.ShapeDtypeStruct((4, 512), f32),
            pltpu.VMEM((4, 2048, 512), bf16),
        ),
        in_specs=[spec(pltpu.VMEM)] * 3 + [spec(pltpu.HBM)] * 6 + [spec(pl.ANY)] * 4,
        out_specs=(spec(pltpu.VMEM),) * 4,
        scratch_shapes=[pltpu.SemaphoreType.DMA((2 + 2 * NX,))],
        compiler_params=PARAMS,
        name="first",
    )(*terms, arrived, *in_hbm(*parts[:6]), *parts[6:])
    return mixed, mine, scales, pltpu.with_memory_space_constraint(halves, pltpu.VMEM)


def begin_kernel(mine_ref, other_ref, total_ref, interp_ref, product_ref, total_out):
    term = added(mine_ref, other_ref)
    total_out[...] = total_ref[...].astype(f32) + term.astype(f32)
    for b in range(4):
        product_ref[b] = times(term, interp_ref, b, 0)


def middle_kernel(order, mine_ref, other_ref, total_ref, product_ref, scales_ref, interp_ref, *outs):
    mixed_ref, out_ref, total_out = outs
    term = added(mine_ref, other_ref)
    total_out[...] = total_ref[...].astype(f32) + term.astype(f32)
    mixed = []
    for b in range(4):
        product = product_ref[b] + times(term, interp_ref, b, 1)
        mixed.append(mix(product, scales_ref, b, order))
        mixed_ref[b] = mixed[b]
    out_ref[...] = back(mixed, interp_ref, 0).astype(bf16)


def finish_kernel(mixed_ref, interp_ref, out_ref):
    mixed = [mixed_ref[b] for b in range(4)]
    out_ref[...] = back(mixed, interp_ref, 1).astype(bf16)


def last_kernel(mine_ref, other_ref, total_0, total_1, product_ref, scales_ref, interp_ref, out_ref):
    c = lax.axis_index("core")
    term = added(mine_ref, other_ref)
    totals = (total_0[...], total_1[...] + term.astype(f32))
    mixed = [
        mix(product_ref[b] + times(term, interp_ref, b, 1), scales_ref, b, TERMS)
        for b in range(4)
    ]
    low, high = slice(0, PIECE), slice(SLAB - PIECE, SLAB)
    for h in range(2):
        acc = back(mixed, interp_ref, h)

        def put(keep, give, h=h, acc=acc):
            kept = (acc[keep] + totals[h][keep]).astype(bf16)
            given = acc[give].astype(bf16)
            for b in range(4):
                out_ref[4 * h + b, :PIECE, :] = kept[:, 256 * b : 256 * b + 256]
                out_ref[4 * h + b, PIECE:, :] = given[:, 256 * b : 256 * b + 256]

        pl.when(c == 1)(lambda put=put: put(low, high))
        pl.when(c == 0)(lambda put=put: put(high, low))


def call_term(kernel, out_shape, *args):
    many = isinstance(out_shape, tuple)
    return pl.pallas_call(
        kernel,
        out_shape=out_shape,
        in_specs=[spec(pltpu.VMEM)] * len(args),
        out_specs=(spec(pltpu.VMEM),) * len(out_shape) if many else spec(pltpu.VMEM),
        compiler_params=PARAMS,
        name="term",
    )(*args)


def end_kernel(back_ref, out_ref):
    for i in range(8):
        start = 8 * TILES[i]
        n = 8 * (TILES[i + 1] - TILES[i])
        owner, partner = (i + 1) % 8, (i + 2) % 8 if i % 2 == 0 else i
        kept = back_ref[owner, :n, :].astype(f32)
        given = back_ref[partner, PIECE : PIECE + n, :].astype(f32)
        out_ref[0, start : start + n, :] = (kept + given).astype(bf16)


def call_end(back):
    return pl.pallas_call(
        end_kernel,
        out_shape=jax.ShapeDtypeStruct((1, ROWS, 256), bf16),
        in_specs=[spec(pltpu.VMEM)],
        out_specs=spec(pltpu.VMEM),
        compiler_params=PARAMS,
        name="end",
    )(back)


def on_device(orbitals, intersection_inv, interp, occ_interp, chol_factors, fields):
    orb = orbitals[0]
    part, rows, inv, orb_v, occ = call_start(interp, intersection_inv[0], orb, occ_interp)
    others = [lax.ppermute(orb, "y", ring(NY, -j)) for j in (1, 2, 3)]
    a_par = swap_core(interp)
    occ_par = swap_core(occ_interp)
    chol_par = swap_core(chol_factors)
    part, *others = lax.optimization_barrier((part, *others))
    part = lax.ppermute(part, "y", ring(NY, 2))
    chol_far = lax.ppermute(chol_factors, "y", ring(NY, 2))
    chol_far_par = swap_core(chol_far)

    weights = call_head(inv, [orb_v, *others], rows, a_par, occ, occ_par)
    mine, other = call_slabs([orb, *others])
    terms = call_join(mine, swap_core(other))
    all_weights = lax.all_to_all(weights, ("z", "x"), 0, 0, tiled=True).reshape(32, 1024)

    far = [part]
    for j in (1, 2, 3):
        far.append(lax.ppermute(part, "x", ring(NX, -j)))
    far_par = []
    for j in range(4):
        far_par.append(swap_core(far[j]))
    near = jnp.concatenate([chol_factors, chol_par], 0).astype(f32)
    partial_bias = jnp.dot(all_weights, near, precision=lax.Precision.HIGHEST)
    biases = to_all(partial_bias, ("y", "core"), 8)
    force_bias, field_part = call_field(
        biases, fields, (chol_factors, chol_par, chol_far, chol_far_par)
    )
    arrived = lax.all_to_all(field_part, ("z", "x"), 0, 0, tiled=True)

    part_shape = jax.ShapeDtypeStruct((SLAB, HALF), bf16)
    total_shape = jax.ShapeDtypeStruct((SLAB, HALF), f32)
    mixed_shape = jax.ShapeDtypeStruct((4, SLAB, 512), bf16)
    product_shape = jax.ShapeDtypeStruct((4, SLAB, 512), f32)
    blocks_shape = jax.ShapeDtypeStruct((8, 2 * PIECE, 256), bf16)
    totals = terms
    mixed, mine_0, scales, interp_v = call_first(
        terms, arrived, (interp, a_par, *far, *far_par)
    )
    for order in range(2, TERMS + 1):
        other_0 = lax.ppermute(mine_0, ("y", "core"), PAIRS)
        mine_1 = call_term(finish_kernel, part_shape, mixed, interp_v)
        other_1 = lax.ppermute(mine_1, ("y", "core"), PAIRS)
        product, total_0 = call_term(
            begin_kernel, (product_shape, total_shape), mine_0, other_0, totals[0], interp_v
        )
        if order < TERMS:
            mixed, mine_0, total_1 = call_term(
                lambda *refs, order=order: middle_kernel(order, *refs),
                (mixed_shape, part_shape, total_shape),
                *(mine_1, other_1, totals[1], product, scales, interp_v),
            )
            totals = (total_0, total_1)
    blocks = call_term(
        last_kernel,
        blocks_shape,
        *(mine_1, other_1, total_0, totals[1], product, scales, interp_v),
    )
    returned = lax.all_to_all(blocks, ("y", "core"), 0, 0, tiled=True)
    return call_end(returned), force_bias


def solution(mesh):
    fine = Mesh(mesh.devices.reshape(NZ, NX, NY, NC), ("z", "x", "y", "core"))
    walk, chol = ("z", "x"), ("y", "core")
    return jax.shard_map(
        on_device,
        mesh=fine,
        in_specs=(
            P(walk, None, chol),
            P(walk, None, None),
            P(None, chol),
            P(None, chol),
            P(chol, walk),
            P(None, walk),
        ),
        out_specs=(P(walk, None, chol), P(None, walk)),
        check_vma=False,
    )
```

```python
import jax
import jax.numpy as jnp
from jax import lax
from jax.experimental import pallas as pl
from jax.experimental.pallas import tpu as pltpu
from jax.sharding import Mesh
from jax.sharding import PartitionSpec as P


TERMS = 4
time_root = 2.2

NZ, NX, NY, NC = 8, 4, 4, 2
ROWS = 400
SLAB = 104
HALF = 1024
PIECE = 56
TILES = (0, 6, 12, 18, 25, 31, 37, 43, 50)
VMEM_LIMIT = 12 * 2**20
f32 = jnp.float32
bf16 = jnp.bfloat16


def ring(n, k):
    return [(i, (i + k) % n) for i in range(n)]


PAIRS = [(i, (i + 1) % 8 if i % 2 else (i - 1) % 8) for i in range(8)]


def swap_core(value):
    return lax.ppermute(value, "core", ring(NC, 1))


def to_all(value, axis, length):
    return lax.all_to_all(
        jnp.broadcast_to(value[None], (length, *value.shape)), axis, 0, 0, tiled=True
    )


def spec(space):
    return pl.BlockSpec(memory_space=space)


def in_hbm(*values):
    return [pltpu.with_memory_space_constraint(v, pltpu.HBM) for v in values]


PARAMS = pltpu.CompilerParams(vmem_limit_bytes=VMEM_LIMIT)


def edge_of(y, c):
    return jnp.where(c == 1, y, (y + 3) % 4)


def start_kernel(interp, inv, orb, occ, part, rows_out, inv_out, orb_out, occ_out, sems):
    x = lax.axis_index("x")
    c = lax.axis_index("core")
    at = pl.multiple_of(x * 512, 512)
    copies = [pltpu.make_async_copy(interp.at[pl.ds(at, 512), :], part, sems.at[0])]
    for y in range(NY):
        at = pl.multiple_of(y * 512 + c * 256, 256)
        rows = interp.at[pl.ds(at, 256), :]
        copies.append(
            pltpu.make_async_copy(rows, rows_out.at[pl.ds(256 * y, 256), :], sems.at[1 + y])
        )
    for k, (a, b) in enumerate(((inv, inv_out), (orb, orb_out), (occ, occ_out))):
        copies.append(pltpu.make_async_copy(a, b, sems.at[5 + k]))
    for copy in copies:
        copy.start()
    for copy in copies:
        copy.wait()


def call_start(interp, inv, orb, occ):
    part, *rest = pl.pallas_call(
        start_kernel,
        out_shape=(
            pltpu.VMEM((512, 512), bf16),
            pltpu.VMEM((1024, 512), bf16),
            pltpu.VMEM((ROWS, ROWS), bf16),
            pltpu.VMEM((ROWS, 256), bf16),
            pltpu.VMEM((ROWS, 512), bf16),
        ),
        in_specs=[spec(pltpu.HBM)] * 4,
        out_specs=(spec(pltpu.VMEM),) * 5,
        scratch_shapes=[pltpu.SemaphoreType.DMA((8,))],
        compiler_params=PARAMS,
        name="start",
    )(*in_hbm(interp, inv, orb, occ))
    return part, *[pltpu.with_memory_space_constraint(r, pltpu.VMEM) for r in rest]


def head_kernel(inv, o0, o1, o2, o3, rows_own, a_par, occ_own, occ_par, weights_ref):
    y = lax.axis_index("y")
    c = lax.axis_index("core")
    sums = [None, None]
    for j, o in enumerate((o0, o1, o2, o3)):
        green = jnp.dot(inv[...], o[...], preferred_element_type=f32).astype(bf16)
        of = (y + j) % NY
        own = rows_own[pl.ds(pl.multiple_of(of * 256, 256), 256), :]
        par = a_par[pl.ds(pl.multiple_of(of * 512 + c * 256, 256), 256), :]
        for k, a in enumerate((own, par)):
            part = jnp.dot(green, a, preferred_element_type=f32)
            sums[k] = part if sums[k] is None else sums[k] + part
    for k, occ in enumerate((occ_own, occ_par)):
        weights = jnp.sum(occ[...].astype(f32) * sums[k], axis=0, keepdims=True)
        weights_ref[:, :, 512 * k : 512 * k + 512] = jnp.broadcast_to(weights, (32, 1, 512))


def call_head(inv, cols, rows_own, a_par, occ_own, occ_par):
    return pl.pallas_call(
        head_kernel,
        out_shape=jax.ShapeDtypeStruct((32, 1, 1024), f32),
        in_specs=[spec(pltpu.VMEM)] * 9,
        out_specs=spec(pltpu.VMEM),
        compiler_params=pltpu.CompilerParams(vmem_limit_bytes=24 * 2**20),
        name="head",
    )(inv, *cols, rows_own, a_par, occ_own, occ_par)


def field_kernel(bias_ref, fields_ref, c0, c1, c2, c3, force_ref, out_ref):
    bias = bias_ref[0]
    for k in range(1, 8):
        bias = bias + bias_ref[k]
    force_ref[...] = bias
    coeff = time_root * (fields_ref[...] - bias)
    coeff = jnp.concatenate([coeff[31 - w : 32 - w] for w in range(32)], 0)
    split = []
    for _ in range(3):
        split.append(coeff.astype(bf16))
        coeff = coeff - split[-1].astype(f32)
    split = jnp.concatenate(split, 0)
    parts = []
    for c in (c0, c1, c2, c3):
        part = lax.dot_general(
            split, c[...], (((1,), (1,)), ((), ())), preferred_element_type=f32
        )
        parts.append(part[:32] + (part[32:64] + part[64:]))
    out_ref[...] = jnp.concatenate(parts, 1).reshape(32, 4, 512).astype(bf16)


def call_field(biases, fields, chols):
    return pl.pallas_call(
        field_kernel,
        out_shape=(
            jax.ShapeDtypeStruct((32, 256), f32),
            jax.ShapeDtypeStruct((32, 4, 512), bf16),
        ),
        in_specs=[spec(pltpu.VMEM)] * 6,
        out_specs=(spec(pltpu.VMEM),) * 2,
        compiler_params=PARAMS,
        name="field",
    )(biases, fields, *chols)


def slab_kernel(o0, o1, o2, o3, mine_ref, other_ref, sems):
    y = lax.axis_index("y")
    c = lax.axis_index("core")
    copies = []
    for k, out in enumerate((mine_ref, other_ref)):
        edge = edge_of(y, c if k == 0 else 1 - c)
        row = edge * 96 + jnp.where(edge >= 2, 8, 0)
        for j, o in enumerate((o0, o1, o2, o3)):
            copy = pltpu.make_async_copy(
                o.at[pl.ds(pl.multiple_of(row, 8), SLAB), :],
                out.at[:, pl.ds(pl.multiple_of(((y + j) % 4) * 256, 256), 256)],
                sems.at[4 * k + j],
            )
            copy.start()
            copies.append(copy)
    for copy in copies:
        copy.wait()


def call_slabs(cols):
    return pl.pallas_call(
        slab_kernel,
        out_shape=(jax.ShapeDtypeStruct((SLAB, 1024), bf16),) * 2,
        in_specs=[spec(pl.ANY)] * 4,
        out_specs=(spec(pl.ANY),) * 2,
        scratch_shapes=[pltpu.SemaphoreType.DMA((8,))],
        compiler_params=PARAMS,
        name="slabs",
    )(*cols)


def join_kernel(own, par, *outs):
    c = lax.axis_index("core")

    def put(first, second):
        for y in range(4):
            cols, out, at = slice(256 * y, 256 * y + 256), outs[y // 2], 512 * (y % 2)
            out[:, at : at + 256] = first[:, cols]
            out[:, at + 256 : at + 512] = second[:, cols]

    pl.when(c == 0)(lambda: put(own, par))
    pl.when(c == 1)(lambda: put(par, own))


def call_join(own, par):
    return pl.pallas_call(
        join_kernel,
        out_shape=(jax.ShapeDtypeStruct((SLAB, HALF), bf16),) * 2,
        in_specs=[spec(pltpu.VMEM)] * 2,
        out_specs=(spec(pltpu.VMEM),) * 2,
        compiler_params=PARAMS,
        name="join",
    )(own, par)


def times(term, interp_ref, b, h):
    rows = interp_ref[b, HALF * h : HALF * h + HALF, :]
    return jnp.dot(term, rows, preferred_element_type=f32)


def back(mixed, interp_ref, h):
    acc = None
    for b in range(4):
        rows = interp_ref[b, HALF * h : HALF * h + HALF, :]
        part = lax.dot_general(mixed[b], rows, (((1,), (1,)), ((), ())), preferred_element_type=f32)
        acc = part if acc is None else acc + part
    return acc


def mix(product, scales_ref, b, order):
    return (product * (scales_ref[b : b + 1, :] / order)).astype(bf16)


def added(mine_ref, other_ref):
    return (mine_ref[...].astype(f32) + other_ref[...].astype(f32)).astype(bf16)


def first_kernel(term_0, term_1, arrived_ref, *refs):
    near, far = refs[:2], (refs[2:6], refs[6:10])
    mixed_ref, out_ref, scales_ref, interp_ref, sems = refs[10:]
    x = lax.axis_index("x")
    copies = [
        [pltpu.make_async_copy(a, interp_ref.at[b], sems.at[b])] for b, a in enumerate(near)
    ]
    for b in range(2):
        copies.append([])
        for j in range(NX):
            at = pl.multiple_of(((x + j) % NX) * 512, 512)
            copies[-1].append(
                pltpu.make_async_copy(
                    far[b][j], interp_ref.at[2 + b, pl.ds(at, 512), :], sems.at[2 + NX * b + j]
                )
            )
    for copy in sum(copies, []):
        copy.start()
    scales_ref[...] = jnp.sum(arrived_ref[...].astype(f32), axis=0)
    mixed = []
    for b in range(4):
        for copy in copies[b]:
            copy.wait()
        product = times(term_0[...], interp_ref, b, 0) + times(term_1[...], interp_ref, b, 1)
        mixed.append(mix(product, scales_ref, b, 1))
        mixed_ref[b] = mixed[b]
    out_ref[...] = back(mixed, interp_ref, 0).astype(bf16)


def call_first(terms, arrived, parts):
    mixed, mine, scales, halves = pl.pallas_call(
        first_kernel,
        out_shape=(
            jax.ShapeDtypeStruct((4, SLAB, 512), bf16),
            jax.ShapeDtypeStruct((SLAB, HALF), bf16),
            jax.ShapeDtypeStruct((4, 512), f32),
            pltpu.VMEM((4, 2048, 512), bf16),
        ),
        in_specs=[spec(pltpu.VMEM)] * 3 + [spec(pltpu.HBM)] * 6 + [spec(pl.ANY)] * 4,
        out_specs=(spec(pltpu.VMEM),) * 4,
        scratch_shapes=[pltpu.SemaphoreType.DMA((2 + 2 * NX,))],
        compiler_params=PARAMS,
        name="first",
    )(*terms, arrived, *in_hbm(*parts[:6]), *parts[6:])
    return mixed, mine, scales, pltpu.with_memory_space_constraint(halves, pltpu.VMEM)


def begin_kernel(mine_ref, other_ref, total_ref, interp_ref, product_ref, total_out):
    term = added(mine_ref, other_ref)
    total_out[...] = total_ref[...].astype(f32) + term.astype(f32)
    for b in range(4):
        product_ref[b] = times(term, interp_ref, b, 0)


def middle_kernel(order, mine_ref, other_ref, total_ref, product_ref, scales_ref, interp_ref, *outs):
    mixed_ref, out_ref, total_out = outs
    term = added(mine_ref, other_ref)
    total_out[...] = total_ref[...].astype(f32) + term.astype(f32)
    mixed = []
    for b in range(4):
        product = product_ref[b] + times(term, interp_ref, b, 1)
        mixed.append(mix(product, scales_ref, b, order))
        mixed_ref[b] = mixed[b]
    out_ref[...] = back(mixed, interp_ref, 0).astype(bf16)


def finish_kernel(mixed_ref, interp_ref, out_ref):
    mixed = [mixed_ref[b] for b in range(4)]
    out_ref[...] = back(mixed, interp_ref, 1).astype(bf16)


def last_kernel(mine_ref, other_ref, total_0, total_1, product_ref, scales_ref, interp_ref, out_ref):
    c = lax.axis_index("core")
    term = added(mine_ref, other_ref)
    totals = (total_0[...], total_1[...] + term.astype(f32))
    mixed = [
        mix(product_ref[b] + times(term, interp_ref, b, 1), scales_ref, b, TERMS)
        for b in range(4)
    ]
    low, high = slice(0, PIECE), slice(SLAB - PIECE, SLAB)
    for h in range(2):
        acc = back(mixed, interp_ref, h)

        def put(keep, give, h=h, acc=acc):
            kept = (acc[keep] + totals[h][keep]).astype(bf16)
            given = acc[give].astype(bf16)
            for b in range(4):
                out_ref[4 * h + b, :PIECE, :] = kept[:, 256 * b : 256 * b + 256]
                out_ref[4 * h + b, PIECE:, :] = given[:, 256 * b : 256 * b + 256]

        pl.when(c == 1)(lambda put=put: put(low, high))
        pl.when(c == 0)(lambda put=put: put(high, low))


def call_term(kernel, out_shape, *args):
    many = isinstance(out_shape, tuple)
    return pl.pallas_call(
        kernel,
        out_shape=out_shape,
        in_specs=[spec(pltpu.VMEM)] * len(args),
        out_specs=(spec(pltpu.VMEM),) * len(out_shape) if many else spec(pltpu.VMEM),
        compiler_params=PARAMS,
        name="term",
    )(*args)


def end_kernel(back_ref, out_ref):
    for i in range(8):
        start = 8 * TILES[i]
        n = 8 * (TILES[i + 1] - TILES[i])
        owner, partner = (i + 1) % 8, (i + 2) % 8 if i % 2 == 0 else i
        kept = back_ref[owner, :n, :].astype(f32)
        given = back_ref[partner, PIECE : PIECE + n, :].astype(f32)
        out_ref[0, start : start + n, :] = (kept + given).astype(bf16)


def call_end(back):
    return pl.pallas_call(
        end_kernel,
        out_shape=jax.ShapeDtypeStruct((1, ROWS, 256), bf16),
        in_specs=[spec(pltpu.VMEM)],
        out_specs=spec(pltpu.VMEM),
        compiler_params=PARAMS,
        name="end",
    )(back)


def on_device(orbitals, intersection_inv, interp, occ_interp, chol_factors, fields):
    orb = orbitals[0]
    part, rows, inv, orb_v, occ = call_start(interp, intersection_inv[0], orb, occ_interp)
    others = [lax.ppermute(orb, "y", ring(NY, -j)) for j in (1, 2, 3)]
    a_par = swap_core(interp)
    occ_par = swap_core(occ_interp)
    chol_par = swap_core(chol_factors)
    part, *others = lax.optimization_barrier((part, *others))
    part = lax.ppermute(part, "y", ring(NY, 2))
    chol_far = lax.ppermute(chol_factors, "y", ring(NY, 2))
    chol_far_par = swap_core(chol_far)

    weights = call_head(inv, [orb_v, *others], rows, a_par, occ, occ_par)
    mine, other = call_slabs([orb, *others])
    terms = call_join(mine, swap_core(other))
    all_weights = lax.all_to_all(weights, ("z", "x"), 0, 0, tiled=True).reshape(32, 1024)

    far = [part]
    for j in (1, 2, 3):
        far.append(lax.ppermute(part, "x", ring(NX, -j)))
    far_par = []
    for j in range(4):
        far_par.append(swap_core(far[j]))
    near = jnp.concatenate([chol_factors, chol_par], 0).astype(f32)
    partial_bias = jnp.dot(all_weights, near, precision=lax.Precision.HIGHEST)
    biases = to_all(partial_bias, ("y", "core"), 8)
    force_bias, field_part = call_field(
        biases, fields, (chol_factors, chol_par, chol_far, chol_far_par)
    )
    arrived = lax.all_to_all(
        field_part, ("z", "x"), 0, 0, tiled=True, axis_index_groups=[list(range(31, -1, -1))]
    )

    part_shape = jax.ShapeDtypeStruct((SLAB, HALF), bf16)
    total_shape = jax.ShapeDtypeStruct((SLAB, HALF), f32)
    mixed_shape = jax.ShapeDtypeStruct((4, SLAB, 512), bf16)
    product_shape = jax.ShapeDtypeStruct((4, SLAB, 512), f32)
    blocks_shape = jax.ShapeDtypeStruct((8, 2 * PIECE, 256), bf16)
    totals = terms
    mixed, mine_0, scales, interp_v = call_first(
        terms, arrived, (interp, a_par, *far, *far_par)
    )
    for order in range(2, TERMS + 1):
        other_0 = lax.ppermute(mine_0, ("y", "core"), PAIRS)
        mine_1 = call_term(finish_kernel, part_shape, mixed, interp_v)
        other_1 = lax.ppermute(mine_1, ("y", "core"), PAIRS)
        product, total_0 = call_term(
            begin_kernel, (product_shape, total_shape), mine_0, other_0, totals[0], interp_v
        )
        if order < TERMS:
            mixed, mine_0, total_1 = call_term(
                lambda *refs, order=order: middle_kernel(order, *refs),
                (mixed_shape, part_shape, total_shape),
                *(mine_1, other_1, totals[1], product, scales, interp_v),
            )
            totals = (total_0, total_1)
    blocks = call_term(
        last_kernel,
        blocks_shape,
        *(mine_1, other_1, total_0, totals[1], product, scales, interp_v),
    )
    returned = lax.all_to_all(blocks, ("y", "core"), 0, 0, tiled=True)
    return call_end(returned), force_bias


def solution(mesh):
    fine = Mesh(mesh.devices.reshape(NZ, NX, NY, NC), ("z", "x", "y", "core"))
    walk, chol = ("z", "x"), ("y", "core")
    return jax.shard_map(
        on_device,
        mesh=fine,
        in_specs=(
            P(walk, None, chol),
            P(walk, None, None),
            P(None, chol),
            P(None, chol),
            P(chol, walk),
            P(None, walk),
        ),
        out_specs=(P(walk, None, chol), P(None, walk)),
        check_vma=False,
    )
```

```python
import jax
import jax.numpy as jnp
from jax import lax
from jax.experimental import pallas as pl
from jax.experimental.pallas import tpu as pltpu
from jax.sharding import Mesh
from jax.sharding import PartitionSpec as P


TERMS = 4
time_root = 2.2

NZ, NX, NY, NC = 8, 4, 4, 2
ROWS = 400
SLAB = 104
HALF = 1024
PIECE = 56
TILES = (0, 6, 12, 18, 25, 31, 37, 43, 50)
VMEM_LIMIT = 12 * 2**20
f32 = jnp.float32
bf16 = jnp.bfloat16


def ring(n, k):
    return [(i, (i + k) % n) for i in range(n)]


Z_ORDER = (4, 3, 5, 2, 6, 1, 7, 0)
WALK_RANKS = [[z * NX + x for z in Z_ORDER for x in range(NX)]]
CHOL_RANKS = [list(range(7, -1, -1))]
PAIRS = [(i, (i + 1) % 8 if i % 2 else (i - 1) % 8) for i in range(8)]


def swap_core(value):
    return lax.ppermute(value, "core", ring(NC, 1))


def spec(space):
    return pl.BlockSpec(memory_space=space)


def in_hbm(*values):
    return [pltpu.with_memory_space_constraint(v, pltpu.HBM) for v in values]


PARAMS = pltpu.CompilerParams(vmem_limit_bytes=VMEM_LIMIT)


def edge_of(y, c):
    return jnp.where(c == 1, y, (y + 3) % 4)


def start_kernel(interp, inv, orb, occ, part, rows_out, inv_out, orb_out, occ_out, sems):
    x = lax.axis_index("x")
    c = lax.axis_index("core")
    at = pl.multiple_of(x * 512, 512)
    copies = [pltpu.make_async_copy(interp.at[pl.ds(at, 512), :], part, sems.at[0])]
    for y in range(NY):
        at = pl.multiple_of(y * 512 + c * 256, 256)
        rows = interp.at[pl.ds(at, 256), :]
        copies.append(
            pltpu.make_async_copy(rows, rows_out.at[pl.ds(256 * y, 256), :], sems.at[1 + y])
        )
    for k, (a, b) in enumerate(((inv, inv_out), (orb, orb_out), (occ, occ_out))):
        copies.append(pltpu.make_async_copy(a, b, sems.at[5 + k]))
    for copy in copies:
        copy.start()
    for copy in copies:
        copy.wait()


def call_start(interp, inv, orb, occ):
    part, *rest = pl.pallas_call(
        start_kernel,
        out_shape=(
            pltpu.VMEM((512, 512), bf16),
            pltpu.VMEM((1024, 512), bf16),
            pltpu.VMEM((ROWS, ROWS), bf16),
            pltpu.VMEM((ROWS, 256), bf16),
            pltpu.VMEM((ROWS, 512), bf16),
        ),
        in_specs=[spec(pltpu.HBM)] * 4,
        out_specs=(spec(pltpu.VMEM),) * 5,
        scratch_shapes=[pltpu.SemaphoreType.DMA((8,))],
        compiler_params=PARAMS,
        name="start",
    )(*in_hbm(interp, inv, orb, occ))
    return part, *[pltpu.with_memory_space_constraint(r, pltpu.VMEM) for r in rest]


def head_kernel(inv, o0, o1, o2, o3, rows_own, a_par, occ_own, occ_par, weights_ref):
    y = lax.axis_index("y")
    c = lax.axis_index("core")
    sums = [None, None]
    for j, o in enumerate((o0, o1, o2, o3)):
        green = jnp.dot(inv[...], o[...], preferred_element_type=f32).astype(bf16)
        of = (y + j) % NY
        own = rows_own[pl.ds(pl.multiple_of(of * 256, 256), 256), :]
        par = a_par[pl.ds(pl.multiple_of(of * 512 + c * 256, 256), 256), :]
        for k, a in enumerate((own, par)):
            part = jnp.dot(green, a, preferred_element_type=f32)
            sums[k] = part if sums[k] is None else sums[k] + part
    for k, occ in enumerate((occ_own, occ_par)):
        weights = jnp.sum(occ[...].astype(f32) * sums[k], axis=0, keepdims=True)
        weights_ref[:, :, 512 * k : 512 * k + 512] = jnp.broadcast_to(weights, (32, 1, 512))


def call_head(inv, cols, rows_own, a_par, occ_own, occ_par):
    return pl.pallas_call(
        head_kernel,
        out_shape=jax.ShapeDtypeStruct((32, 1, 1024), f32),
        in_specs=[spec(pltpu.VMEM)] * 9,
        out_specs=spec(pltpu.VMEM),
        compiler_params=pltpu.CompilerParams(vmem_limit_bytes=24 * 2**20),
        name="head",
    )(inv, *cols, rows_own, a_par, occ_own, occ_par)


def field_kernel(bias_ref, fields_ref, c0, c1, c2, c3, force_ref, out_ref):
    bias = bias_ref[0]
    for k in range(1, 8):
        bias = bias + bias_ref[k]
    for rank, z in enumerate(Z_ORDER):
        force_ref[NX * z : NX * z + NX, :] = bias[NX * rank : NX * rank + NX]
    fields = jnp.concatenate([fields_ref[NX * z : NX * z + NX, :] for z in Z_ORDER], 0)
    coeff = time_root * (fields - bias)
    split = []
    for _ in range(3):
        split.append(coeff.astype(bf16))
        coeff = coeff - split[-1].astype(f32)
    split = jnp.concatenate(split, 0)
    parts = []
    for c in (c0, c1, c2, c3):
        part = lax.dot_general(
            split, c[...], (((1,), (1,)), ((), ())), preferred_element_type=f32
        )
        parts.append(part[:32] + (part[32:64] + part[64:]))
    out_ref[...] = jnp.concatenate(parts, 1).reshape(32, 4, 512).astype(bf16)


def call_field(biases, fields, chols):
    return pl.pallas_call(
        field_kernel,
        out_shape=(
            jax.ShapeDtypeStruct((32, 256), f32),
            jax.ShapeDtypeStruct((32, 4, 512), bf16),
        ),
        in_specs=[spec(pltpu.VMEM)] * 6,
        out_specs=(spec(pltpu.VMEM),) * 2,
        compiler_params=PARAMS,
        name="field",
    )(biases, fields, *chols)


def slab_kernel(o0, o1, o2, o3, mine_ref, other_ref, sems):
    y = lax.axis_index("y")
    c = lax.axis_index("core")
    copies = []
    for k, out in enumerate((mine_ref, other_ref)):
        edge = edge_of(y, c if k == 0 else 1 - c)
        row = edge * 96 + jnp.where(edge >= 2, 8, 0)
        for j, o in enumerate((o0, o1, o2, o3)):
            copy = pltpu.make_async_copy(
                o.at[pl.ds(pl.multiple_of(row, 8), SLAB), :],
                out.at[:, pl.ds(pl.multiple_of(((y + j) % 4) * 256, 256), 256)],
                sems.at[4 * k + j],
            )
            copy.start()
            copies.append(copy)
    for copy in copies:
        copy.wait()


def call_slabs(cols):
    return pl.pallas_call(
        slab_kernel,
        out_shape=(jax.ShapeDtypeStruct((SLAB, 1024), bf16),) * 2,
        in_specs=[spec(pl.ANY)] * 4,
        out_specs=(spec(pl.ANY),) * 2,
        scratch_shapes=[pltpu.SemaphoreType.DMA((8,))],
        compiler_params=PARAMS,
        name="slabs",
    )(*cols)


def join_kernel(own, par, *outs):
    c = lax.axis_index("core")

    def put(first, second):
        for y in range(4):
            cols, out, at = slice(256 * y, 256 * y + 256), outs[y // 2], 512 * (y % 2)
            out[:, at : at + 256] = first[:, cols]
            out[:, at + 256 : at + 512] = second[:, cols]

    pl.when(c == 0)(lambda: put(own, par))
    pl.when(c == 1)(lambda: put(par, own))


def call_join(own, par):
    return pl.pallas_call(
        join_kernel,
        out_shape=(jax.ShapeDtypeStruct((SLAB, HALF), bf16),) * 2,
        in_specs=[spec(pltpu.VMEM)] * 2,
        out_specs=(spec(pltpu.VMEM),) * 2,
        compiler_params=PARAMS,
        name="join",
    )(own, par)


def times(term, interp_ref, b, h):
    rows = interp_ref[b, HALF * h : HALF * h + HALF, :]
    return jnp.dot(term, rows, preferred_element_type=f32)


def back(mixed, interp_ref, h):
    acc = None
    for b in range(4):
        rows = interp_ref[b, HALF * h : HALF * h + HALF, :]
        part = lax.dot_general(mixed[b], rows, (((1,), (1,)), ((), ())), preferred_element_type=f32)
        acc = part if acc is None else acc + part
    return acc


def mix(product, scales_ref, b, order):
    return (product * (scales_ref[b : b + 1, :] / order)).astype(bf16)


def added(mine_ref, other_ref):
    return (mine_ref[...].astype(f32) + other_ref[...].astype(f32)).astype(bf16)


def first_kernel(term_0, term_1, arrived_ref, *refs):
    near, far = refs[:2], (refs[2:6], refs[6:10])
    mixed_ref, out_ref, scales_ref, interp_ref, sems = refs[10:]
    x = lax.axis_index("x")
    copies = [
        [pltpu.make_async_copy(a, interp_ref.at[b], sems.at[b])] for b, a in enumerate(near)
    ]
    for b in range(2):
        copies.append([])
        for j in range(NX):
            at = pl.multiple_of(((x + j) % NX) * 512, 512)
            copies[-1].append(
                pltpu.make_async_copy(
                    far[b][j], interp_ref.at[2 + b, pl.ds(at, 512), :], sems.at[2 + NX * b + j]
                )
            )
    for copy in sum(copies, []):
        copy.start()
    scales_ref[...] = jnp.sum(arrived_ref[...].astype(f32), axis=0)
    mixed = []
    for b in range(4):
        for copy in copies[b]:
            copy.wait()
        product = times(term_0[...], interp_ref, b, 0) + times(term_1[...], interp_ref, b, 1)
        mixed.append(mix(product, scales_ref, b, 1))
        mixed_ref[b] = mixed[b]
    out_ref[...] = back(mixed, interp_ref, 0).astype(bf16)


def call_first(terms, arrived, parts):
    mixed, mine, scales, halves = pl.pallas_call(
        first_kernel,
        out_shape=(
            jax.ShapeDtypeStruct((4, SLAB, 512), bf16),
            jax.ShapeDtypeStruct((SLAB, HALF), bf16),
            jax.ShapeDtypeStruct((4, 512), f32),
            pltpu.VMEM((4, 2048, 512), bf16),
        ),
        in_specs=[spec(pltpu.VMEM)] * 3 + [spec(pltpu.HBM)] * 6 + [spec(pl.ANY)] * 4,
        out_specs=(spec(pltpu.VMEM),) * 4,
        scratch_shapes=[pltpu.SemaphoreType.DMA((2 + 2 * NX,))],
        compiler_params=PARAMS,
        name="first",
    )(*terms, arrived, *in_hbm(*parts[:6]), *parts[6:])
    return mixed, mine, scales, pltpu.with_memory_space_constraint(halves, pltpu.VMEM)


def begin_kernel(mine_ref, other_ref, total_ref, interp_ref, product_ref, total_out):
    term = added(mine_ref, other_ref)
    total_out[...] = total_ref[...].astype(f32) + term.astype(f32)
    for b in range(4):
        product_ref[b] = times(term, interp_ref, b, 0)


def middle_kernel(order, mine_ref, other_ref, total_ref, product_ref, scales_ref, interp_ref, *outs):
    mixed_ref, out_ref, total_out = outs
    term = added(mine_ref, other_ref)
    total_out[...] = total_ref[...].astype(f32) + term.astype(f32)
    mixed = []
    for b in range(4):
        product = product_ref[b] + times(term, interp_ref, b, 1)
        mixed.append(mix(product, scales_ref, b, order))
        mixed_ref[b] = mixed[b]
    out_ref[...] = back(mixed, interp_ref, 0).astype(bf16)


def finish_kernel(mixed_ref, interp_ref, out_ref):
    mixed = [mixed_ref[b] for b in range(4)]
    out_ref[...] = back(mixed, interp_ref, 1).astype(bf16)


def last_kernel(mine_ref, other_ref, total_0, total_1, product_ref, scales_ref, interp_ref, out_ref):
    c = lax.axis_index("core")
    term = added(mine_ref, other_ref)
    totals = (total_0[...], total_1[...] + term.astype(f32))
    mixed = [
        mix(product_ref[b] + times(term, interp_ref, b, 1), scales_ref, b, TERMS)
        for b in range(4)
    ]
    low, high = slice(0, PIECE), slice(SLAB - PIECE, SLAB)
    for h in range(2):
        acc = back(mixed, interp_ref, h)

        def put(keep, give, h=h, acc=acc):
            kept = (acc[keep] + totals[h][keep]).astype(bf16)
            given = acc[give].astype(bf16)
            for b in range(4):
                out_ref[7 - 4 * h - b, :PIECE, :] = kept[:, 256 * b : 256 * b + 256]
                out_ref[7 - 4 * h - b, PIECE:, :] = given[:, 256 * b : 256 * b + 256]

        pl.when(c == 1)(lambda put=put: put(low, high))
        pl.when(c == 0)(lambda put=put: put(high, low))


def call_term(kernel, out_shape, *args):
    many = isinstance(out_shape, tuple)
    return pl.pallas_call(
        kernel,
        out_shape=out_shape,
        in_specs=[spec(pltpu.VMEM)] * len(args),
        out_specs=(spec(pltpu.VMEM),) * len(out_shape) if many else spec(pltpu.VMEM),
        compiler_params=PARAMS,
        name="term",
    )(*args)


def end_kernel(back_ref, out_ref):
    for i in range(8):
        start = 8 * TILES[i]
        n = 8 * (TILES[i + 1] - TILES[i])
        owner, partner = (i + 1) % 8, (i + 2) % 8 if i % 2 == 0 else i
        kept = back_ref[7 - owner, :n, :].astype(f32)
        given = back_ref[7 - partner, PIECE : PIECE + n, :].astype(f32)
        out_ref[0, start : start + n, :] = (kept + given).astype(bf16)


def call_end(back):
    return pl.pallas_call(
        end_kernel,
        out_shape=jax.ShapeDtypeStruct((1, ROWS, 256), bf16),
        in_specs=[spec(pltpu.VMEM)],
        out_specs=spec(pltpu.VMEM),
        compiler_params=PARAMS,
        name="end",
    )(back)


def on_device(orbitals, intersection_inv, interp, occ_interp, chol_factors, fields):
    orb = orbitals[0]
    part, rows, inv, orb_v, occ = call_start(interp, intersection_inv[0], orb, occ_interp)
    others = [lax.ppermute(orb, "y", ring(NY, -j)) for j in (1, 2, 3)]
    a_par = swap_core(interp)
    occ_par = swap_core(occ_interp)
    chol_par = swap_core(chol_factors)
    part, *others = lax.optimization_barrier((part, *others))
    part = lax.ppermute(part, "y", ring(NY, 2))
    chol_far = lax.ppermute(chol_factors, "y", ring(NY, 2))
    chol_far_par = swap_core(chol_far)

    weights = call_head(inv, [orb_v, *others], rows, a_par, occ, occ_par)
    mine, other = call_slabs([orb, *others])
    terms = call_join(mine, swap_core(other))
    all_weights = lax.all_to_all(
        weights, ("z", "x"), 0, 0, tiled=True, axis_index_groups=WALK_RANKS
    ).reshape(32, 1024)

    far = [part]
    for j in (1, 2, 3):
        far.append(lax.ppermute(part, "x", ring(NX, -j)))
    far_par = []
    for j in range(4):
        far_par.append(swap_core(far[j]))
    near = jnp.concatenate([chol_factors, chol_par], 0).astype(f32)
    partial_bias = jnp.dot(all_weights, near, precision=lax.Precision.HIGHEST)
    biases = lax.all_to_all(
        jnp.broadcast_to(partial_bias[None], (8, 32, 256)),
        ("y", "core"),
        0,
        0,
        tiled=True,
        axis_index_groups=CHOL_RANKS,
    )
    force_bias, field_part = call_field(
        biases, fields, (chol_factors, chol_par, chol_far, chol_far_par)
    )
    arrived = lax.all_to_all(field_part, ("z", "x"), 0, 0, tiled=True, axis_index_groups=WALK_RANKS)

    part_shape = jax.ShapeDtypeStruct((SLAB, HALF), bf16)
    total_shape = jax.ShapeDtypeStruct((SLAB, HALF), f32)
    mixed_shape = jax.ShapeDtypeStruct((4, SLAB, 512), bf16)
    product_shape = jax.ShapeDtypeStruct((4, SLAB, 512), f32)
    blocks_shape = jax.ShapeDtypeStruct((8, 2 * PIECE, 256), bf16)
    totals = terms
    mixed, mine_0, scales, interp_v = call_first(
        terms, arrived, (interp, a_par, *far, *far_par)
    )
    for order in range(2, TERMS + 1):
        other_0 = lax.ppermute(mine_0, ("y", "core"), PAIRS)
        mine_1 = call_term(finish_kernel, part_shape, mixed, interp_v)
        other_1 = lax.ppermute(mine_1, ("y", "core"), PAIRS)
        product, total_0 = call_term(
            begin_kernel, (product_shape, total_shape), mine_0, other_0, totals[0], interp_v
        )
        if order < TERMS:
            mixed, mine_0, total_1 = call_term(
                lambda *refs, order=order: middle_kernel(order, *refs),
                (mixed_shape, part_shape, total_shape),
                *(mine_1, other_1, totals[1], product, scales, interp_v),
            )
            totals = (total_0, total_1)
    blocks = call_term(
        last_kernel,
        blocks_shape,
        *(mine_1, other_1, total_0, totals[1], product, scales, interp_v),
    )
    returned = lax.all_to_all(blocks, ("y", "core"), 0, 0, tiled=True, axis_index_groups=CHOL_RANKS)
    return call_end(returned), force_bias


def solution(mesh):
    fine = Mesh(mesh.devices.reshape(NZ, NX, NY, NC), ("z", "x", "y", "core"))
    walk, chol = ("z", "x"), ("y", "core")
    return jax.shard_map(
        on_device,
        mesh=fine,
        in_specs=(
            P(walk, None, chol),
            P(walk, None, None),
            P(None, chol),
            P(None, chol),
            P(chol, walk),
            P(None, walk),
        ),
        out_specs=(P(walk, None, chol), P(None, walk)),
        check_vma=False,
    )
```

```python
import jax
import jax.numpy as jnp
from jax import lax
from jax.experimental import pallas as pl
from jax.experimental.pallas import tpu as pltpu
from jax.sharding import Mesh
from jax.sharding import PartitionSpec as P


TERMS = 4
time_root = 2.2

NZ, NX, NY, NC = 8, 4, 4, 2
ROWS = 400
SLAB = 104
HALF = 1024
PIECE = 56
TILES = (0, 6, 12, 18, 25, 31, 37, 43, 50)
VMEM_LIMIT = 12 * 2**20
f32 = jnp.float32
bf16 = jnp.bfloat16


def ring(n, k):
    return [(i, (i + k) % n) for i in range(n)]


Z_ORDER = (4, 3, 5, 2, 6, 1, 7, 0)
WALK_RANKS = [[z * NX + x for z in Z_ORDER for x in range(NX)]]
CHOL_RANKS = [list(range(7, -1, -1))]
PAIRS = [(i, (i + 1) % 8 if i % 2 else (i - 1) % 8) for i in range(8)]


def swap_core(value):
    return lax.ppermute(value, "core", ring(NC, 1))


def spec(space):
    return pl.BlockSpec(memory_space=space)


def in_hbm(*values):
    return [pltpu.with_memory_space_constraint(v, pltpu.HBM) for v in values]


PARAMS = pltpu.CompilerParams(vmem_limit_bytes=VMEM_LIMIT)


def edge_of(y, c):
    return jnp.where(c == 1, y, (y + 3) % 4)


def start_kernel(interp, inv, orb, occ, part, rows_out, inv_out, orb_out, occ_out, sems):
    x = lax.axis_index("x")
    c = lax.axis_index("core")
    at = pl.multiple_of(x * 512, 512)
    copies = [pltpu.make_async_copy(interp.at[pl.ds(at, 512), :], part, sems.at[0])]
    for y in range(NY):
        at = pl.multiple_of(y * 512 + c * 256, 256)
        rows = interp.at[pl.ds(at, 256), :]
        copies.append(
            pltpu.make_async_copy(rows, rows_out.at[pl.ds(256 * y, 256), :], sems.at[1 + y])
        )
    for k, (a, b) in enumerate(((inv, inv_out), (orb, orb_out), (occ, occ_out))):
        copies.append(pltpu.make_async_copy(a, b, sems.at[5 + k]))
    for copy in copies:
        copy.start()
    for copy in copies:
        copy.wait()


def call_start(interp, inv, orb, occ):
    part, *rest = pl.pallas_call(
        start_kernel,
        out_shape=(
            pltpu.VMEM((512, 512), bf16),
            pltpu.VMEM((1024, 512), bf16),
            pltpu.VMEM((ROWS, ROWS), bf16),
            pltpu.VMEM((ROWS, 256), bf16),
            pltpu.VMEM((ROWS, 512), bf16),
        ),
        in_specs=[spec(pltpu.HBM)] * 4,
        out_specs=(spec(pltpu.VMEM),) * 5,
        scratch_shapes=[pltpu.SemaphoreType.DMA((8,))],
        compiler_params=PARAMS,
        name="start",
    )(*in_hbm(interp, inv, orb, occ))
    return part, *[pltpu.with_memory_space_constraint(r, pltpu.VMEM) for r in rest]


def head_kernel(inv, o0, o1, o2, o3, rows_own, a_par, occ_own, occ_par, weights_ref):
    y = lax.axis_index("y")
    c = lax.axis_index("core")
    sums = [None, None]
    for j, o in enumerate((o0, o1, o2, o3)):
        green = jnp.dot(inv[...], o[...], preferred_element_type=f32).astype(bf16)
        of = (y + j) % NY
        own = rows_own[pl.ds(pl.multiple_of(of * 256, 256), 256), :]
        par = a_par[pl.ds(pl.multiple_of(of * 512 + c * 256, 256), 256), :]
        for k, a in enumerate((own, par)):
            part = jnp.dot(green, a, preferred_element_type=f32)
            sums[k] = part if sums[k] is None else sums[k] + part
    for k, occ in enumerate((occ_own, occ_par)):
        weights = jnp.sum(occ[...].astype(f32) * sums[k], axis=0, keepdims=True)
        weights_ref[:, :, 512 * k : 512 * k + 512] = jnp.broadcast_to(weights, (32, 1, 512))


def call_head(inv, cols, rows_own, a_par, occ_own, occ_par):
    return pl.pallas_call(
        head_kernel,
        out_shape=jax.ShapeDtypeStruct((32, 1, 1024), f32),
        in_specs=[spec(pltpu.VMEM)] * 9,
        out_specs=spec(pltpu.VMEM),
        compiler_params=pltpu.CompilerParams(vmem_limit_bytes=24 * 2**20),
        name="head",
    )(inv, *cols, rows_own, a_par, occ_own, occ_par)


def field_kernel(bias_ref, fields_ref, c0, c1, c2, c3, force_ref, out_ref):
    bias = bias_ref[0]
    for k in range(1, 8):
        bias = bias + bias_ref[k]
    for rank, z in enumerate(Z_ORDER):
        force_ref[NX * z : NX * z + NX, :] = bias[NX * rank : NX * rank + NX]
    fields = jnp.concatenate([fields_ref[NX * z : NX * z + NX, :] for z in Z_ORDER], 0)
    coeff = time_root * (fields - bias)
    split = []
    for _ in range(3):
        split.append(coeff.astype(bf16))
        coeff = coeff - split[-1].astype(f32)
    split = jnp.concatenate(split, 0)
    parts = []
    for c in (c0, c1, c2, c3):
        part = lax.dot_general(
            split, c[...], (((1,), (1,)), ((), ())), preferred_element_type=f32
        )
        parts.append(part[:32] + (part[32:64] + part[64:]))
    out_ref[...] = jnp.concatenate(parts, 1).reshape(32, 4, 512).astype(bf16)


def call_field(biases, fields, chols):
    return pl.pallas_call(
        field_kernel,
        out_shape=(
            jax.ShapeDtypeStruct((32, 256), f32),
            jax.ShapeDtypeStruct((32, 4, 512), bf16),
        ),
        in_specs=[spec(pltpu.VMEM)] * 6,
        out_specs=(spec(pltpu.VMEM),) * 2,
        compiler_params=PARAMS,
        name="field",
    )(biases, fields, *chols)


def slab_kernel(o0, o1, o2, o3, mine_ref, other_ref, sems):
    y = lax.axis_index("y")
    c = lax.axis_index("core")
    copies = []
    for k, out in enumerate((mine_ref, other_ref)):
        edge = edge_of(y, c if k == 0 else 1 - c)
        row = edge * 96 + jnp.where(edge >= 2, 8, 0)
        for j, o in enumerate((o0, o1, o2, o3)):
            copy = pltpu.make_async_copy(
                o.at[pl.ds(pl.multiple_of(row, 8), SLAB), :],
                out.at[:, pl.ds(pl.multiple_of(((y + j) % 4) * 256, 256), 256)],
                sems.at[4 * k + j],
            )
            copy.start()
            copies.append(copy)
    for copy in copies:
        copy.wait()


def call_slabs(cols):
    return pl.pallas_call(
        slab_kernel,
        out_shape=(jax.ShapeDtypeStruct((SLAB, 1024), bf16),) * 2,
        in_specs=[spec(pl.ANY)] * 4,
        out_specs=(spec(pl.ANY),) * 2,
        scratch_shapes=[pltpu.SemaphoreType.DMA((8,))],
        compiler_params=PARAMS,
        name="slabs",
    )(*cols)


def join_kernel(own, par, *outs):
    c = lax.axis_index("core")

    def put(first, second):
        for y in range(4):
            cols, out, at = slice(256 * y, 256 * y + 256), outs[y // 2], 512 * (y % 2)
            out[:, at : at + 256] = first[:, cols]
            out[:, at + 256 : at + 512] = second[:, cols]

    pl.when(c == 0)(lambda: put(own, par))
    pl.when(c == 1)(lambda: put(par, own))


def call_join(own, par):
    return pl.pallas_call(
        join_kernel,
        out_shape=(jax.ShapeDtypeStruct((SLAB, HALF), bf16),) * 2,
        in_specs=[spec(pltpu.VMEM)] * 2,
        out_specs=(spec(pltpu.VMEM),) * 2,
        compiler_params=PARAMS,
        name="join",
    )(own, par)


def times(term, interp_ref, b, h):
    rows = interp_ref[b, HALF * h : HALF * h + HALF, :]
    return jnp.dot(term, rows, preferred_element_type=f32)


def back(mixed, interp_ref, h):
    acc = None
    for b in range(4):
        rows = interp_ref[b, HALF * h : HALF * h + HALF, :]
        part = lax.dot_general(mixed[b], rows, (((1,), (1,)), ((), ())), preferred_element_type=f32)
        acc = part if acc is None else acc + part
    return acc


def mix(product, scales_ref, b, order):
    return (product * (scales_ref[b : b + 1, :] / order)).astype(bf16)


def added(mine_ref, other_ref):
    return (mine_ref[...].astype(f32) + other_ref[...].astype(f32)).astype(bf16)


def first_kernel(term_0, term_1, arrived_ref, *refs):
    near, far = refs[:2], (refs[2:6], refs[6:10])
    mixed_ref, out_ref, scales_ref, interp_ref, sems = refs[10:]
    x = lax.axis_index("x")
    copies = [
        [pltpu.make_async_copy(a, interp_ref.at[b], sems.at[b])] for b, a in enumerate(near)
    ]
    for b in range(2):
        copies.append([])
        for j in range(NX):
            at = pl.multiple_of(((x + j) % NX) * 512, 512)
            copies[-1].append(
                pltpu.make_async_copy(
                    far[b][j], interp_ref.at[2 + b, pl.ds(at, 512), :], sems.at[2 + NX * b + j]
                )
            )
    for copy in sum(copies, []):
        copy.start()
    scales_ref[...] = jnp.sum(arrived_ref[...].astype(f32), axis=0)
    mixed = []
    for b in range(4):
        for copy in copies[b]:
            copy.wait()
        product = times(term_0[...], interp_ref, b, 0) + times(term_1[...], interp_ref, b, 1)
        mixed.append(mix(product, scales_ref, b, 1))
        mixed_ref[b] = mixed[b]
    out_ref[...] = back(mixed, interp_ref, 0).astype(bf16)


def call_first(terms, arrived, parts):
    mixed, mine, scales, halves = pl.pallas_call(
        first_kernel,
        out_shape=(
            jax.ShapeDtypeStruct((4, SLAB, 512), bf16),
            jax.ShapeDtypeStruct((SLAB, HALF), bf16),
            jax.ShapeDtypeStruct((4, 512), f32),
            pltpu.VMEM((4, 2048, 512), bf16),
        ),
        in_specs=[spec(pltpu.VMEM)] * 3 + [spec(pltpu.HBM)] * 6 + [spec(pl.ANY)] * 4,
        out_specs=(spec(pltpu.VMEM),) * 4,
        scratch_shapes=[pltpu.SemaphoreType.DMA((2 + 2 * NX,))],
        compiler_params=PARAMS,
        name="first",
    )(*terms, arrived, *in_hbm(*parts[:6]), *parts[6:])
    return mixed, mine, scales, pltpu.with_memory_space_constraint(halves, pltpu.VMEM)


def begin_kernel(mine_ref, other_ref, total_ref, interp_ref, product_ref, total_out):
    term = added(mine_ref, other_ref)
    total_out[...] = total_ref[...].astype(f32) + term.astype(f32)
    for b in range(4):
        product_ref[b] = times(term, interp_ref, b, 0)


def middle_kernel(order, mine_ref, other_ref, total_ref, product_ref, scales_ref, interp_ref, *outs):
    mixed_ref, out_ref, total_out = outs
    term = added(mine_ref, other_ref)
    total_out[...] = total_ref[...].astype(f32) + term.astype(f32)
    mixed = []
    for b in range(4):
        product = product_ref[b] + times(term, interp_ref, b, 1)
        mixed.append(mix(product, scales_ref, b, order))
        mixed_ref[b] = mixed[b]
    out_ref[...] = back(mixed, interp_ref, 0).astype(bf16)


def finish_kernel(mixed_ref, interp_ref, out_ref):
    mixed = [mixed_ref[b] for b in range(4)]
    out_ref[...] = back(mixed, interp_ref, 1).astype(bf16)


def last_kernel(mine_ref, other_ref, total_0, total_1, product_ref, scales_ref, interp_ref, out_ref):
    c = lax.axis_index("core")
    term = added(mine_ref, other_ref)
    totals = (total_0[...], total_1[...] + term.astype(f32))
    mixed = [
        mix(product_ref[b] + times(term, interp_ref, b, 1), scales_ref, b, TERMS)
        for b in range(4)
    ]
    low, high = slice(0, PIECE), slice(SLAB - PIECE, SLAB)
    for h in range(2):
        acc = back(mixed, interp_ref, h)

        def put(keep, give, h=h, acc=acc):
            kept = (acc[keep] + totals[h][keep]).astype(bf16)
            given = acc[give].astype(bf16)
            for b in range(4):
                out_ref[7 - 4 * h - b, :PIECE, :] = kept[:, 256 * b : 256 * b + 256]
                out_ref[7 - 4 * h - b, PIECE:, :] = given[:, 256 * b : 256 * b + 256]

        pl.when(c == 1)(lambda put=put: put(low, high))
        pl.when(c == 0)(lambda put=put: put(high, low))


def call_term(kernel, out_shape, *args):
    many = isinstance(out_shape, tuple)
    return pl.pallas_call(
        kernel,
        out_shape=out_shape,
        in_specs=[spec(pltpu.VMEM)] * len(args),
        out_specs=(spec(pltpu.VMEM),) * len(out_shape) if many else spec(pltpu.VMEM),
        compiler_params=PARAMS,
        name="term",
    )(*args)


def end_kernel(back_ref, out_ref):
    for i in range(8):
        start = 8 * TILES[i]
        n = 8 * (TILES[i + 1] - TILES[i])
        owner, partner = (i + 1) % 8, (i + 2) % 8 if i % 2 == 0 else i
        kept = back_ref[7 - owner, :n, :].astype(f32)
        given = back_ref[7 - partner, PIECE : PIECE + n, :].astype(f32)
        out_ref[0, start : start + n, :] = (kept + given).astype(bf16)


def call_end(back):
    return pl.pallas_call(
        end_kernel,
        out_shape=jax.ShapeDtypeStruct((1, ROWS, 256), bf16),
        in_specs=[spec(pltpu.VMEM)],
        out_specs=spec(pltpu.VMEM),
        compiler_params=PARAMS,
        name="end",
    )(back)


def on_device(orbitals, intersection_inv, interp, occ_interp, chol_factors, fields):
    orb = orbitals[0]
    part, rows, inv, orb_v, occ = call_start(interp, intersection_inv[0], orb, occ_interp)
    others = []
    for j in (1, 2, 3):
        others.append(lax.ppermute(orb, "y", ring(NY, -j)))
    a_par = swap_core(interp)
    occ_par = swap_core(occ_interp)
    chol_par = swap_core(chol_factors)
    part, others[0], others[2] = lax.optimization_barrier((part, others[0], others[2]))
    part = lax.ppermute(part, "y", ring(NY, 2))
    chol_far = lax.ppermute(chol_factors, "y", ring(NY, 2))
    chol_far_par = swap_core(chol_far)

    weights = call_head(inv, [orb_v, *others], rows, a_par, occ, occ_par)
    mine, other = call_slabs([orb, *others])
    other = swap_core(other)
    terms = call_join(mine, other)
    all_weights = lax.all_to_all(
        weights, ("z", "x"), 0, 0, tiled=True, axis_index_groups=WALK_RANKS
    ).reshape(32, 1024)

    far = [part]
    for j in (1, 2, 3):
        far.append(lax.ppermute(part, "x", ring(NX, -j)))
    far_par = []
    for j in range(4):
        far_par.append(swap_core(far[j]))
    near = jnp.concatenate([chol_factors, chol_par], 0).astype(f32)
    partial_bias = jnp.dot(all_weights, near, precision=lax.Precision.HIGHEST)
    biases = lax.all_to_all(
        jnp.broadcast_to(partial_bias[None], (8, 32, 256)),
        ("y", "core"),
        0,
        0,
        tiled=True,
        axis_index_groups=CHOL_RANKS,
    )
    force_bias, field_part = call_field(
        biases, fields, (chol_factors, chol_par, chol_far, chol_far_par)
    )
    arrived = lax.all_to_all(field_part, ("z", "x"), 0, 0, tiled=True, axis_index_groups=WALK_RANKS)

    part_shape = jax.ShapeDtypeStruct((SLAB, HALF), bf16)
    total_shape = jax.ShapeDtypeStruct((SLAB, HALF), f32)
    mixed_shape = jax.ShapeDtypeStruct((4, SLAB, 512), bf16)
    product_shape = jax.ShapeDtypeStruct((4, SLAB, 512), f32)
    blocks_shape = jax.ShapeDtypeStruct((8, 2 * PIECE, 256), bf16)
    totals = terms
    mixed, mine_0, scales, interp_v = call_first(
        terms, arrived, (interp, a_par, *far, *far_par)
    )
    for order in range(2, TERMS + 1):
        other_0 = lax.ppermute(mine_0, ("y", "core"), PAIRS)
        mine_1 = call_term(finish_kernel, part_shape, mixed, interp_v)
        other_1 = lax.ppermute(mine_1, ("y", "core"), PAIRS)
        product, total_0 = call_term(
            begin_kernel, (product_shape, total_shape), mine_0, other_0, totals[0], interp_v
        )
        if order < TERMS:
            mixed, mine_0, total_1 = call_term(
                lambda *refs, order=order: middle_kernel(order, *refs),
                (mixed_shape, part_shape, total_shape),
                *(mine_1, other_1, totals[1], product, scales, interp_v),
            )
            totals = (total_0, total_1)
    blocks = call_term(
        last_kernel,
        blocks_shape,
        *(mine_1, other_1, total_0, totals[1], product, scales, interp_v),
    )
    returned = lax.all_to_all(blocks, ("y", "core"), 0, 0, tiled=True, axis_index_groups=CHOL_RANKS)
    return call_end(returned), force_bias


def solution(mesh):
    fine = Mesh(mesh.devices.reshape(NZ, NX, NY, NC), ("z", "x", "y", "core"))
    walk, chol = ("z", "x"), ("y", "core")
    return jax.shard_map(
        on_device,
        mesh=fine,
        in_specs=(
            P(walk, None, chol),
            P(walk, None, None),
            P(None, chol),
            P(None, chol),
            P(chol, walk),
            P(None, walk),
        ),
        out_specs=(P(walk, None, chol), P(None, walk)),
        check_vma=False,
    )
```

```python
import jax
import jax.numpy as jnp
from jax import lax
from jax.experimental import pallas as pl
from jax.experimental.pallas import tpu as pltpu
from jax.sharding import Mesh
from jax.sharding import PartitionSpec as P


TERMS = 4
time_root = 2.2

NZ, NX, NY, NC = 8, 4, 4, 2
ROWS = 400
SLAB = 104
HALF = 1024
PIECE = 56
TILES = (0, 6, 12, 18, 25, 31, 37, 43, 50)
VMEM_LIMIT = 12 * 2**20
f32 = jnp.float32
bf16 = jnp.bfloat16


def ring(n, k):
    return [(i, (i + k) % n) for i in range(n)]


Z_ORDER = (4, 3, 5, 2, 6, 1, 7, 0)
WALK_RANKS = [[z * NX + x for z in Z_ORDER for x in range(NX)]]
CHOL_RANKS = [list(range(7, -1, -1))]
OWNERS = (0, 2, 5, 3, 4, 6, 1, 7)
PAIRS = [(OWNERS[i], OWNERS[i ^ 1]) for i in range(8)]


def swap_core(value):
    return lax.ppermute(value, "core", ring(NC, 1))


def spec(space):
    return pl.BlockSpec(memory_space=space)


def in_hbm(*values):
    return [pltpu.with_memory_space_constraint(v, pltpu.HBM) for v in values]


PARAMS = pltpu.CompilerParams(vmem_limit_bytes=VMEM_LIMIT)


def edge_of(y, c):
    return jnp.where(c == 0, y // 2 * 2, jnp.where((y == 1) | (y == 2), 1, 3))


def start_kernel(interp, inv, orb, occ, part, rows_out, inv_out, orb_out, occ_out, sems):
    x = lax.axis_index("x")
    c = lax.axis_index("core")
    at = pl.multiple_of(x * 512, 512)
    copies = [pltpu.make_async_copy(interp.at[pl.ds(at, 512), :], part, sems.at[0])]
    for y in range(NY):
        at = pl.multiple_of(y * 512 + c * 256, 256)
        rows = interp.at[pl.ds(at, 256), :]
        copies.append(
            pltpu.make_async_copy(rows, rows_out.at[pl.ds(256 * y, 256), :], sems.at[1 + y])
        )
    for k, (a, b) in enumerate(((inv, inv_out), (orb, orb_out), (occ, occ_out))):
        copies.append(pltpu.make_async_copy(a, b, sems.at[5 + k]))
    for copy in copies:
        copy.start()
    for copy in copies:
        copy.wait()


def call_start(interp, inv, orb, occ):
    part, *rest = pl.pallas_call(
        start_kernel,
        out_shape=(
            pltpu.VMEM((512, 512), bf16),
            pltpu.VMEM((1024, 512), bf16),
            pltpu.VMEM((ROWS, ROWS), bf16),
            pltpu.VMEM((ROWS, 256), bf16),
            pltpu.VMEM((ROWS, 512), bf16),
        ),
        in_specs=[spec(pltpu.HBM)] * 4,
        out_specs=(spec(pltpu.VMEM),) * 5,
        scratch_shapes=[pltpu.SemaphoreType.DMA((8,))],
        compiler_params=PARAMS,
        name="start",
    )(*in_hbm(interp, inv, orb, occ))
    return part, *[pltpu.with_memory_space_constraint(r, pltpu.VMEM) for r in rest]


def head_kernel(inv, o0, o1, o2, o3, rows_own, a_par, occ_own, occ_par, weights_ref):
    y = lax.axis_index("y")
    c = lax.axis_index("core")
    sums = [None, None]
    for j, o in enumerate((o0, o1, o2, o3)):
        green = jnp.dot(inv[...], o[...], preferred_element_type=f32).astype(bf16)
        of = (y + j) % NY
        own = rows_own[pl.ds(pl.multiple_of(of * 256, 256), 256), :]
        par = a_par[pl.ds(pl.multiple_of(of * 512 + c * 256, 256), 256), :]
        for k, a in enumerate((own, par)):
            part = jnp.dot(green, a, preferred_element_type=f32)
            sums[k] = part if sums[k] is None else sums[k] + part
    for k, occ in enumerate((occ_own, occ_par)):
        weights = jnp.sum(occ[...].astype(f32) * sums[k], axis=0, keepdims=True)
        weights_ref[:, :, 512 * k : 512 * k + 512] = jnp.broadcast_to(weights, (32, 1, 512))


def call_head(inv, cols, rows_own, a_par, occ_own, occ_par):
    return pl.pallas_call(
        head_kernel,
        out_shape=jax.ShapeDtypeStruct((32, 1, 1024), f32),
        in_specs=[spec(pltpu.VMEM)] * 9,
        out_specs=spec(pltpu.VMEM),
        compiler_params=pltpu.CompilerParams(vmem_limit_bytes=24 * 2**20),
        name="head",
    )(inv, *cols, rows_own, a_par, occ_own, occ_par)


def field_kernel(bias_ref, fields_ref, c0, c1, c2, c3, force_ref, out_ref):
    bias = bias_ref[0]
    for k in range(1, 8):
        bias = bias + bias_ref[k]
    for rank, z in enumerate(Z_ORDER):
        force_ref[NX * z : NX * z + NX, :] = bias[NX * rank : NX * rank + NX]
    fields = jnp.concatenate([fields_ref[NX * z : NX * z + NX, :] for z in Z_ORDER], 0)
    coeff = time_root * (fields - bias)
    split = []
    for _ in range(3):
        split.append(coeff.astype(bf16))
        coeff = coeff - split[-1].astype(f32)
    split = jnp.concatenate(split, 0)
    parts = []
    for c in (c0, c1, c2, c3):
        part = lax.dot_general(
            split, c[...], (((1,), (1,)), ((), ())), preferred_element_type=f32
        )
        parts.append(part[:32] + (part[32:64] + part[64:]))
    out_ref[...] = jnp.concatenate(parts, 1).reshape(32, 4, 512).astype(bf16)


def call_field(biases, fields, chols):
    return pl.pallas_call(
        field_kernel,
        out_shape=(
            jax.ShapeDtypeStruct((32, 256), f32),
            jax.ShapeDtypeStruct((32, 4, 512), bf16),
        ),
        in_specs=[spec(pltpu.VMEM)] * 6,
        out_specs=(spec(pltpu.VMEM),) * 2,
        compiler_params=PARAMS,
        name="field",
    )(biases, fields, *chols)


def slab_kernel(o0, o1, o2, o3, mine_ref, other_ref, sems):
    y = lax.axis_index("y")
    c = lax.axis_index("core")
    copies = []
    for k, out in enumerate((mine_ref, other_ref)):
        edge = edge_of(y, c if k == 0 else 1 - c)
        row = edge * 96 + jnp.where(edge >= 2, 8, 0)
        for j, o in enumerate((o0, o1, o2, o3)):
            copy = pltpu.make_async_copy(
                o.at[pl.ds(pl.multiple_of(row, 8), SLAB), :],
                out.at[:, pl.ds(pl.multiple_of(((y + j) % 4) * 256, 256), 256)],
                sems.at[4 * k + j],
            )
            copy.start()
            copies.append(copy)
    for copy in copies:
        copy.wait()


def call_slabs(cols):
    return pl.pallas_call(
        slab_kernel,
        out_shape=(jax.ShapeDtypeStruct((SLAB, 1024), bf16),) * 2,
        in_specs=[spec(pl.ANY)] * 4,
        out_specs=(spec(pl.ANY),) * 2,
        scratch_shapes=[pltpu.SemaphoreType.DMA((8,))],
        compiler_params=PARAMS,
        name="slabs",
    )(*cols)


def join_kernel(own, par, *outs):
    c = lax.axis_index("core")

    def put(first, second):
        for y in range(4):
            cols, out, at = slice(256 * y, 256 * y + 256), outs[y // 2], 512 * (y % 2)
            out[:, at : at + 256] = first[:, cols]
            out[:, at + 256 : at + 512] = second[:, cols]

    pl.when(c == 0)(lambda: put(own, par))
    pl.when(c == 1)(lambda: put(par, own))


def call_join(own, par):
    return pl.pallas_call(
        join_kernel,
        out_shape=(jax.ShapeDtypeStruct((SLAB, HALF), bf16),) * 2,
        in_specs=[spec(pltpu.VMEM)] * 2,
        out_specs=(spec(pltpu.VMEM),) * 2,
        compiler_params=PARAMS,
        name="join",
    )(own, par)


def times(term, interp_ref, b, h):
    rows = interp_ref[b, HALF * h : HALF * h + HALF, :]
    return jnp.dot(term, rows, preferred_element_type=f32)


def back(mixed, interp_ref, h):
    acc = None
    for b in range(4):
        rows = interp_ref[b, HALF * h : HALF * h + HALF, :]
        part = lax.dot_general(mixed[b], rows, (((1,), (1,)), ((), ())), preferred_element_type=f32)
        acc = part if acc is None else acc + part
    return acc


def mix(product, scales_ref, b, order):
    return (product * (scales_ref[b : b + 1, :] / order)).astype(bf16)


def added(mine_ref, other_ref):
    return (mine_ref[...].astype(f32) + other_ref[...].astype(f32)).astype(bf16)


def first_kernel(term_0, term_1, arrived_ref, *refs):
    near, far = refs[:2], (refs[2:6], refs[6:10])
    mixed_ref, out_ref, scales_ref, interp_ref, sems = refs[10:]
    x = lax.axis_index("x")
    copies = [
        [pltpu.make_async_copy(a, interp_ref.at[b], sems.at[b])] for b, a in enumerate(near)
    ]
    for b in range(2):
        copies.append([])
        for j in range(NX):
            at = pl.multiple_of(((x + j) % NX) * 512, 512)
            copies[-1].append(
                pltpu.make_async_copy(
                    far[b][j], interp_ref.at[2 + b, pl.ds(at, 512), :], sems.at[2 + NX * b + j]
                )
            )
    for copy in sum(copies, []):
        copy.start()
    scales_ref[...] = jnp.sum(arrived_ref[...].astype(f32), axis=0)
    mixed = []
    for b in range(4):
        for copy in copies[b]:
            copy.wait()
        product = times(term_0[...], interp_ref, b, 0) + times(term_1[...], interp_ref, b, 1)
        mixed.append(mix(product, scales_ref, b, 1))
        mixed_ref[b] = mixed[b]
    out_ref[...] = back(mixed, interp_ref, 0).astype(bf16)


def call_first(terms, arrived, parts):
    mixed, mine, scales, halves = pl.pallas_call(
        first_kernel,
        out_shape=(
            jax.ShapeDtypeStruct((4, SLAB, 512), bf16),
            jax.ShapeDtypeStruct((SLAB, HALF), bf16),
            jax.ShapeDtypeStruct((4, 512), f32),
            pltpu.VMEM((4, 2048, 512), bf16),
        ),
        in_specs=[spec(pltpu.VMEM)] * 3 + [spec(pltpu.HBM)] * 6 + [spec(pl.ANY)] * 4,
        out_specs=(spec(pltpu.VMEM),) * 4,
        scratch_shapes=[pltpu.SemaphoreType.DMA((2 + 2 * NX,))],
        compiler_params=PARAMS,
        name="first",
    )(*terms, arrived, *in_hbm(*parts[:6]), *parts[6:])
    return mixed, mine, scales, pltpu.with_memory_space_constraint(halves, pltpu.VMEM)


def begin_kernel(mine_ref, other_ref, total_ref, interp_ref, product_ref, total_out):
    term = added(mine_ref, other_ref)
    total_out[...] = total_ref[...].astype(f32) + term.astype(f32)
    for b in range(4):
        product_ref[b] = times(term, interp_ref, b, 0)


def middle_kernel(order, mine_ref, other_ref, total_ref, product_ref, scales_ref, interp_ref, *outs):
    mixed_ref, out_ref, total_out = outs
    term = added(mine_ref, other_ref)
    total_out[...] = total_ref[...].astype(f32) + term.astype(f32)
    mixed = []
    for b in range(4):
        product = product_ref[b] + times(term, interp_ref, b, 1)
        mixed.append(mix(product, scales_ref, b, order))
        mixed_ref[b] = mixed[b]
    out_ref[...] = back(mixed, interp_ref, 0).astype(bf16)


def finish_kernel(mixed_ref, interp_ref, out_ref):
    mixed = [mixed_ref[b] for b in range(4)]
    out_ref[...] = back(mixed, interp_ref, 1).astype(bf16)


def last_kernel(mine_ref, other_ref, total_0, total_1, product_ref, scales_ref, interp_ref, out_ref):
    y = lax.axis_index("y")
    term = added(mine_ref, other_ref)
    totals = (total_0[...], total_1[...] + term.astype(f32))
    mixed = [
        mix(product_ref[b] + times(term, interp_ref, b, 1), scales_ref, b, TERMS)
        for b in range(4)
    ]
    low, high = slice(0, PIECE), slice(SLAB - PIECE, SLAB)
    for h in range(2):
        acc = back(mixed, interp_ref, h)

        def put(keep, give, h=h, acc=acc):
            kept = (acc[keep] + totals[h][keep]).astype(bf16)
            given = acc[give].astype(bf16)
            for b in range(4):
                out_ref[7 - 4 * h - b, :PIECE, :] = kept[:, 256 * b : 256 * b + 256]
                out_ref[7 - 4 * h - b, PIECE:, :] = given[:, 256 * b : 256 * b + 256]

        pl.when(y % 2 == 0)(lambda put=put: put(low, high))
        pl.when(y % 2 == 1)(lambda put=put: put(high, low))


def call_term(kernel, out_shape, *args):
    many = isinstance(out_shape, tuple)
    return pl.pallas_call(
        kernel,
        out_shape=out_shape,
        in_specs=[spec(pltpu.VMEM)] * len(args),
        out_specs=(spec(pltpu.VMEM),) * len(out_shape) if many else spec(pltpu.VMEM),
        compiler_params=PARAMS,
        name="term",
    )(*args)


def end_kernel(back_ref, out_ref):
    for i in range(8):
        start = 8 * TILES[i]
        n = 8 * (TILES[i + 1] - TILES[i])
        owner, partner = OWNERS[i], OWNERS[i ^ 1]
        kept = back_ref[7 - owner, :n, :].astype(f32)
        given = back_ref[7 - partner, PIECE : PIECE + n, :].astype(f32)
        out_ref[0, start : start + n, :] = (kept + given).astype(bf16)


def call_end(back):
    return pl.pallas_call(
        end_kernel,
        out_shape=jax.ShapeDtypeStruct((1, ROWS, 256), bf16),
        in_specs=[spec(pltpu.VMEM)],
        out_specs=spec(pltpu.VMEM),
        compiler_params=PARAMS,
        name="end",
    )(back)


def on_device(orbitals, intersection_inv, interp, occ_interp, chol_factors, fields):
    orb = orbitals[0]
    part, rows, inv, orb_v, occ = call_start(interp, intersection_inv[0], orb, occ_interp)
    others = []
    for j in (1, 2, 3):
        others.append(lax.ppermute(orb, "y", ring(NY, -j)))
    a_par = swap_core(interp)
    occ_par = swap_core(occ_interp)
    chol_par = swap_core(chol_factors)
    part, others[0], others[2] = lax.optimization_barrier((part, others[0], others[2]))
    part = lax.ppermute(part, "y", ring(NY, 2))
    chol_far = lax.ppermute(chol_factors, "y", ring(NY, 2))
    chol_far_par = swap_core(chol_far)

    weights = call_head(inv, [orb_v, *others], rows, a_par, occ, occ_par)
    mine, other = call_slabs([orb, *others])
    other = swap_core(other)
    terms = call_join(mine, other)
    all_weights = lax.all_to_all(
        weights, ("z", "x"), 0, 0, tiled=True, axis_index_groups=WALK_RANKS
    ).reshape(32, 1024)

    far = [part]
    for j in (1, 2, 3):
        far.append(lax.ppermute(part, "x", ring(NX, -j)))
    far_par = []
    for j in range(4):
        far_par.append(swap_core(far[j]))
    near = jnp.concatenate([chol_factors, chol_par], 0).astype(f32)
    partial_bias = jnp.dot(all_weights, near, precision=lax.Precision.HIGHEST)
    biases = lax.all_to_all(
        jnp.broadcast_to(partial_bias[None], (8, 32, 256)),
        ("y", "core"),
        0,
        0,
        tiled=True,
        axis_index_groups=CHOL_RANKS,
    )
    force_bias, field_part = call_field(
        biases, fields, (chol_factors, chol_par, chol_far, chol_far_par)
    )
    arrived = lax.all_to_all(field_part, ("z", "x"), 0, 0, tiled=True, axis_index_groups=WALK_RANKS)

    part_shape = jax.ShapeDtypeStruct((SLAB, HALF), bf16)
    total_shape = jax.ShapeDtypeStruct((SLAB, HALF), f32)
    mixed_shape = jax.ShapeDtypeStruct((4, SLAB, 512), bf16)
    product_shape = jax.ShapeDtypeStruct((4, SLAB, 512), f32)
    blocks_shape = jax.ShapeDtypeStruct((8, 2 * PIECE, 256), bf16)
    totals = terms
    mixed, mine_0, scales, interp_v = call_first(
        terms, arrived, (interp, a_par, *far, *far_par)
    )
    for order in range(2, TERMS + 1):
        other_0 = lax.ppermute(mine_0, ("y", "core"), PAIRS)
        mine_1 = call_term(finish_kernel, part_shape, mixed, interp_v)
        other_1 = lax.ppermute(mine_1, ("y", "core"), PAIRS)
        product, total_0 = call_term(
            begin_kernel, (product_shape, total_shape), mine_0, other_0, totals[0], interp_v
        )
        if order < TERMS:
            mixed, mine_0, total_1 = call_term(
                lambda *refs, order=order: middle_kernel(order, *refs),
                (mixed_shape, part_shape, total_shape),
                *(mine_1, other_1, totals[1], product, scales, interp_v),
            )
            totals = (total_0, total_1)
    blocks = call_term(
        last_kernel,
        blocks_shape,
        *(mine_1, other_1, total_0, totals[1], product, scales, interp_v),
    )
    returned = lax.all_to_all(blocks, ("y", "core"), 0, 0, tiled=True, axis_index_groups=CHOL_RANKS)
    return call_end(returned), force_bias


def solution(mesh):
    fine = Mesh(mesh.devices.reshape(NZ, NX, NY, NC), ("z", "x", "y", "core"))
    walk, chol = ("z", "x"), ("y", "core")
    return jax.shard_map(
        on_device,
        mesh=fine,
        in_specs=(
            P(walk, None, chol),
            P(walk, None, None),
            P(None, chol),
            P(None, chol),
            P(chol, walk),
            P(None, walk),
        ),
        out_specs=(P(walk, None, chol), P(None, walk)),
        check_vma=False,
    )
```

```python
import jax
import jax.numpy as jnp
from jax import lax
from jax.experimental import pallas as pl
from jax.experimental.pallas import tpu as pltpu
from jax.sharding import Mesh
from jax.sharding import PartitionSpec as P


TERMS = 4
time_root = 2.2

NZ, NX, NY, NC = 8, 4, 4, 2
ROWS = 400
SLAB = 104
HALF = 1024
PIECE = 56
TILES = (0, 6, 12, 18, 25, 31, 37, 43, 50)
VMEM_LIMIT = 12 * 2**20
f32 = jnp.float32
bf16 = jnp.bfloat16


def ring(n, k):
    return [(i, (i + k) % n) for i in range(n)]


Z_ORDER = (4, 3, 5, 2, 6, 1, 7, 0)
WALK_RANKS = [[z * NX + x for z in Z_ORDER for x in range(NX)]]
CHOL_RANKS = [list(range(7, -1, -1))]
OWNERS = (0, 2, 5, 3, 4, 6, 1, 7)
PAIRS = [(OWNERS[i], OWNERS[i ^ 1]) for i in range(8)]


def swap_core(value):
    return lax.ppermute(value, "core", ring(NC, 1))


def spec(space):
    return pl.BlockSpec(memory_space=space)


def in_hbm(*values):
    return [pltpu.with_memory_space_constraint(v, pltpu.HBM) for v in values]


PARAMS = pltpu.CompilerParams(vmem_limit_bytes=VMEM_LIMIT)


def edge_of(y, c):
    return jnp.where(c == 0, y // 2 * 2, jnp.where((y == 1) | (y == 2), 1, 3))


def start_kernel(interp, inv, orb, occ, part, rows_out, inv_out, orb_out, occ_out, sems):
    x = lax.axis_index("x")
    c = lax.axis_index("core")
    at = pl.multiple_of(x * 512, 512)
    copies = [pltpu.make_async_copy(interp.at[pl.ds(at, 512), :], part, sems.at[0])]
    for y in range(NY):
        at = pl.multiple_of(y * 512 + c * 256, 256)
        rows = interp.at[pl.ds(at, 256), :]
        copies.append(
            pltpu.make_async_copy(rows, rows_out.at[pl.ds(256 * y, 256), :], sems.at[1 + y])
        )
    for k, (a, b) in enumerate(((inv, inv_out), (orb, orb_out), (occ, occ_out))):
        copies.append(pltpu.make_async_copy(a, b, sems.at[5 + k]))
    for copy in copies:
        copy.start()
    for copy in copies:
        copy.wait()


def call_start(interp, inv, orb, occ):
    part, *rest = pl.pallas_call(
        start_kernel,
        out_shape=(
            pltpu.VMEM((512, 512), bf16),
            pltpu.VMEM((1024, 512), bf16),
            pltpu.VMEM((ROWS, ROWS), bf16),
            pltpu.VMEM((ROWS, 256), bf16),
            pltpu.VMEM((ROWS, 512), bf16),
        ),
        in_specs=[spec(pltpu.HBM)] * 4,
        out_specs=(spec(pltpu.VMEM),) * 5,
        scratch_shapes=[pltpu.SemaphoreType.DMA((8,))],
        compiler_params=PARAMS,
        name="start",
    )(*in_hbm(interp, inv, orb, occ))
    return part, *[pltpu.with_memory_space_constraint(r, pltpu.VMEM) for r in rest]


def head_kernel(inv, o0, o1, o2, o3, rows_own, a_par, occ_own, occ_par, weights_ref):
    y = lax.axis_index("y")
    c = lax.axis_index("core")
    sums = [None, None]
    for j, o in enumerate((o0, o1, o2, o3)):
        green = jnp.dot(inv[...], o[...], preferred_element_type=f32).astype(bf16)
        of = (y + j) % NY
        own = rows_own[pl.ds(pl.multiple_of(of * 256, 256), 256), :]
        par = a_par[pl.ds(pl.multiple_of(of * 512 + c * 256, 256), 256), :]
        for k, a in enumerate((own, par)):
            part = jnp.dot(green, a, preferred_element_type=f32)
            sums[k] = part if sums[k] is None else sums[k] + part
    for k, occ in enumerate((occ_own, occ_par)):
        weights = jnp.sum(occ[...].astype(f32) * sums[k], axis=0, keepdims=True)
        weights_ref[:, :, 512 * k : 512 * k + 512] = jnp.broadcast_to(weights, (32, 1, 512))


def call_head(inv, cols, rows_own, a_par, occ_own, occ_par):
    return pl.pallas_call(
        head_kernel,
        out_shape=jax.ShapeDtypeStruct((32, 1, 1024), f32),
        in_specs=[spec(pltpu.VMEM)] * 9,
        out_specs=spec(pltpu.VMEM),
        compiler_params=pltpu.CompilerParams(vmem_limit_bytes=24 * 2**20),
        name="head",
    )(inv, *cols, rows_own, a_par, occ_own, occ_par)


def field_kernel(bias_ref, fields_ref, c0, c1, c2, c3, force_ref, out_ref):
    bias = bias_ref[0]
    for k in range(1, 8):
        bias = bias + bias_ref[k]
    for rank, z in enumerate(Z_ORDER):
        force_ref[NX * z : NX * z + NX, :] = bias[NX * rank : NX * rank + NX]
    fields = jnp.concatenate([fields_ref[NX * z : NX * z + NX, :] for z in Z_ORDER], 0)
    coeff = time_root * (fields - bias)
    split = []
    for _ in range(3):
        split.append(coeff.astype(bf16))
        coeff = coeff - split[-1].astype(f32)
    split = jnp.concatenate(split, 0)
    parts = []
    for c in (c0, c1, c2, c3):
        part = lax.dot_general(
            split, c[...], (((1,), (1,)), ((), ())), preferred_element_type=f32
        )
        parts.append(part[:32] + (part[32:64] + part[64:]))
    out_ref[...] = jnp.concatenate(parts, 1).reshape(32, 4, 512).astype(bf16)


def call_field(biases, fields, chols):
    return pl.pallas_call(
        field_kernel,
        out_shape=(
            jax.ShapeDtypeStruct((32, 256), f32),
            jax.ShapeDtypeStruct((32, 4, 512), bf16),
        ),
        in_specs=[spec(pltpu.VMEM)] * 6,
        out_specs=(spec(pltpu.VMEM),) * 2,
        compiler_params=PARAMS,
        name="field",
    )(biases, fields, *chols)


def slab_kernel(o0, o1, o2, o3, mine_ref, other_ref, sems):
    y = lax.axis_index("y")
    c = lax.axis_index("core")
    copies = []
    for k, out in enumerate((mine_ref, other_ref)):
        edge = edge_of(y, c if k == 0 else 1 - c)
        row = edge * 96 + jnp.where(edge >= 2, 8, 0)
        for j, o in enumerate((o0, o1, o2, o3)):
            copy = pltpu.make_async_copy(
                o.at[pl.ds(pl.multiple_of(row, 8), SLAB), :],
                out.at[:, pl.ds(pl.multiple_of(((y + j) % 4) * 256, 256), 256)],
                sems.at[4 * k + j],
            )
            copy.start()
            copies.append(copy)
    for copy in copies:
        copy.wait()


def call_slabs(cols):
    return pl.pallas_call(
        slab_kernel,
        out_shape=(jax.ShapeDtypeStruct((SLAB, 1024), bf16),) * 2,
        in_specs=[spec(pl.ANY)] * 4,
        out_specs=(spec(pl.ANY),) * 2,
        scratch_shapes=[pltpu.SemaphoreType.DMA((8,))],
        compiler_params=PARAMS,
        name="slabs",
    )(*cols)


def join_kernel(own, par, *outs):
    c = lax.axis_index("core")

    def put(first, second):
        for y in range(4):
            cols, out, at = slice(256 * y, 256 * y + 256), outs[y // 2], 512 * (y % 2)
            out[:, at : at + 256] = first[:, cols]
            out[:, at + 256 : at + 512] = second[:, cols]

    pl.when(c == 0)(lambda: put(own, par))
    pl.when(c == 1)(lambda: put(par, own))


def call_join(own, par):
    return pl.pallas_call(
        join_kernel,
        out_shape=(jax.ShapeDtypeStruct((SLAB, HALF), bf16),) * 2,
        in_specs=[spec(pltpu.VMEM)] * 2,
        out_specs=(spec(pltpu.VMEM),) * 2,
        compiler_params=PARAMS,
        name="join",
    )(own, par)


def times(term, interp_ref, b, h):
    rows = interp_ref[b, HALF * h : HALF * h + HALF, :]
    return jnp.dot(term, rows, preferred_element_type=f32)


def back(mixed, interp_ref, h):
    acc = None
    for b in range(4):
        rows = interp_ref[b, HALF * h : HALF * h + HALF, :]
        part = lax.dot_general(mixed[b], rows, (((1,), (1,)), ((), ())), preferred_element_type=f32)
        acc = part if acc is None else acc + part
    return acc


def mix(product, scales_ref, b, order):
    return (product * (scales_ref[b : b + 1, :] / order)).astype(bf16)


def added(mine_ref, other_ref):
    return (mine_ref[...].astype(f32) + other_ref[...].astype(f32)).astype(bf16)


def first_kernel(term_0, term_1, arrived_ref, *refs):
    near, far = refs[:2], (refs[2:6], refs[6:10])
    mixed_ref, out_ref, scales_ref, interp_ref, sems = refs[10:]
    x = lax.axis_index("x")
    copies = [
        [pltpu.make_async_copy(a, interp_ref.at[b], sems.at[b])] for b, a in enumerate(near)
    ]
    for b in range(2):
        copies.append([])
        for j in range(NX):
            at = pl.multiple_of(((x + j) % NX) * 512, 512)
            copies[-1].append(
                pltpu.make_async_copy(
                    far[b][j], interp_ref.at[2 + b, pl.ds(at, 512), :], sems.at[2 + NX * b + j]
                )
            )
    for b in (3, 0, 1, 2):
        for copy in copies[b]:
            copy.start()
    scales_ref[...] = jnp.sum(arrived_ref[...].astype(f32), axis=0)
    mixed = [None] * 4
    for b in (3, 0, 1, 2):
        for copy in copies[b]:
            copy.wait()
        product = times(term_0[...], interp_ref, b, 0) + times(term_1[...], interp_ref, b, 1)
        mixed[b] = mix(product, scales_ref, b, 1)
        mixed_ref[b] = mixed[b]
    out_ref[...] = back(mixed, interp_ref, 0).astype(bf16)


def call_first(terms, arrived, parts):
    mixed, mine, scales, halves = pl.pallas_call(
        first_kernel,
        out_shape=(
            jax.ShapeDtypeStruct((4, SLAB, 512), bf16),
            jax.ShapeDtypeStruct((SLAB, HALF), bf16),
            jax.ShapeDtypeStruct((4, 512), f32),
            pltpu.VMEM((4, 2048, 512), bf16),
        ),
        in_specs=[spec(pltpu.VMEM)] * 3 + [spec(pltpu.HBM)] * 6 + [spec(pl.ANY)] * 4,
        out_specs=(spec(pltpu.VMEM),) * 4,
        scratch_shapes=[pltpu.SemaphoreType.DMA((2 + 2 * NX,))],
        compiler_params=PARAMS,
        name="first",
    )(*terms, arrived, *in_hbm(*parts[:6]), *parts[6:])
    return mixed, mine, scales, pltpu.with_memory_space_constraint(halves, pltpu.VMEM)


def begin_kernel(mine_ref, other_ref, total_ref, interp_ref, product_ref, total_out):
    term = added(mine_ref, other_ref)
    total_out[...] = total_ref[...].astype(f32) + term.astype(f32)
    for b in range(4):
        product_ref[b] = times(term, interp_ref, b, 0)


def middle_kernel(order, mine_ref, other_ref, total_ref, product_ref, scales_ref, interp_ref, *outs):
    mixed_ref, out_ref, total_out = outs
    term = added(mine_ref, other_ref)
    total_out[...] = total_ref[...].astype(f32) + term.astype(f32)
    mixed = []
    for b in range(4):
        product = product_ref[b] + times(term, interp_ref, b, 1)
        mixed.append(mix(product, scales_ref, b, order))
        mixed_ref[b] = mixed[b]
    out_ref[...] = back(mixed, interp_ref, 0).astype(bf16)


def finish_kernel(mixed_ref, interp_ref, out_ref):
    mixed = [mixed_ref[b] for b in range(4)]
    out_ref[...] = back(mixed, interp_ref, 1).astype(bf16)


def last_kernel(mine_ref, other_ref, total_0, total_1, product_ref, scales_ref, interp_ref, out_ref):
    y = lax.axis_index("y")
    term = added(mine_ref, other_ref)
    totals = (total_0[...], total_1[...] + term.astype(f32))
    mixed = [
        mix(product_ref[b] + times(term, interp_ref, b, 1), scales_ref, b, TERMS)
        for b in range(4)
    ]
    low, high = slice(0, PIECE), slice(SLAB - PIECE, SLAB)
    for h in range(2):
        acc = back(mixed, interp_ref, h)

        def put(keep, give, h=h, acc=acc):
            kept = (acc[keep] + totals[h][keep]).astype(bf16)
            given = acc[give].astype(bf16)
            for b in range(4):
                out_ref[7 - 4 * h - b, :PIECE, :] = kept[:, 256 * b : 256 * b + 256]
                out_ref[7 - 4 * h - b, PIECE:, :] = given[:, 256 * b : 256 * b + 256]

        pl.when(y % 2 == 0)(lambda put=put: put(low, high))
        pl.when(y % 2 == 1)(lambda put=put: put(high, low))


def call_term(kernel, out_shape, *args):
    many = isinstance(out_shape, tuple)
    return pl.pallas_call(
        kernel,
        out_shape=out_shape,
        in_specs=[spec(pltpu.VMEM)] * len(args),
        out_specs=(spec(pltpu.VMEM),) * len(out_shape) if many else spec(pltpu.VMEM),
        compiler_params=PARAMS,
        name="term",
    )(*args)


def end_kernel(back_ref, out_ref):
    for i in range(8):
        start = 8 * TILES[i]
        n = 8 * (TILES[i + 1] - TILES[i])
        owner, partner = OWNERS[i], OWNERS[i ^ 1]
        kept = back_ref[7 - owner, :n, :].astype(f32)
        given = back_ref[7 - partner, PIECE : PIECE + n, :].astype(f32)
        out_ref[0, start : start + n, :] = (kept + given).astype(bf16)


def call_end(back):
    return pl.pallas_call(
        end_kernel,
        out_shape=jax.ShapeDtypeStruct((1, ROWS, 256), bf16),
        in_specs=[spec(pltpu.VMEM)],
        out_specs=spec(pltpu.VMEM),
        compiler_params=PARAMS,
        name="end",
    )(back)


def on_device(orbitals, intersection_inv, interp, occ_interp, chol_factors, fields):
    orb = orbitals[0]
    part, rows, inv, orb_v, occ = call_start(interp, intersection_inv[0], orb, occ_interp)
    others = []
    for j in (1, 2, 3):
        others.append(lax.ppermute(orb, "y", ring(NY, -j)))
    a_par = swap_core(interp)
    occ_par = swap_core(occ_interp)
    chol_par = swap_core(chol_factors)
    part, others[0], others[2] = lax.optimization_barrier((part, others[0], others[2]))
    part = lax.ppermute(part, "y", ring(NY, 2))
    chol_far = lax.ppermute(chol_factors, "y", ring(NY, 2))
    chol_far_par = swap_core(chol_far)

    weights = call_head(inv, [orb_v, *others], rows, a_par, occ, occ_par)
    mine, other = call_slabs([orb, *others])
    other = swap_core(other)
    terms = call_join(mine, other)
    all_weights = lax.all_to_all(
        weights, ("z", "x"), 0, 0, tiled=True, axis_index_groups=WALK_RANKS
    ).reshape(32, 1024)

    far = [part]
    for j in (1, 2, 3):
        far.append(lax.ppermute(part, "x", ring(NX, -j)))
    far_par = []
    for j in range(4):
        far_par.append(swap_core(far[j]))
    near = jnp.concatenate([chol_factors, chol_par], 0).astype(f32)
    partial_bias = jnp.dot(all_weights, near, precision=lax.Precision.HIGHEST)
    biases = lax.all_to_all(
        jnp.broadcast_to(partial_bias[None], (8, 32, 256)),
        ("y", "core"),
        0,
        0,
        tiled=True,
        axis_index_groups=CHOL_RANKS,
    )
    force_bias, field_part = call_field(
        biases, fields, (chol_factors, chol_par, chol_far, chol_far_par)
    )
    arrived = lax.all_to_all(field_part, ("z", "x"), 0, 0, tiled=True, axis_index_groups=WALK_RANKS)

    part_shape = jax.ShapeDtypeStruct((SLAB, HALF), bf16)
    total_shape = jax.ShapeDtypeStruct((SLAB, HALF), f32)
    mixed_shape = jax.ShapeDtypeStruct((4, SLAB, 512), bf16)
    product_shape = jax.ShapeDtypeStruct((4, SLAB, 512), f32)
    blocks_shape = jax.ShapeDtypeStruct((8, 2 * PIECE, 256), bf16)
    totals = terms
    mixed, mine_0, scales, interp_v = call_first(
        terms, arrived, (interp, a_par, *far, *far_par)
    )
    for order in range(2, TERMS + 1):
        other_0 = lax.ppermute(mine_0, ("y", "core"), PAIRS)
        mine_1 = call_term(finish_kernel, part_shape, mixed, interp_v)
        other_1 = lax.ppermute(mine_1, ("y", "core"), PAIRS)
        product, total_0 = call_term(
            begin_kernel, (product_shape, total_shape), mine_0, other_0, totals[0], interp_v
        )
        if order < TERMS:
            mixed, mine_0, total_1 = call_term(
                lambda *refs, order=order: middle_kernel(order, *refs),
                (mixed_shape, part_shape, total_shape),
                *(mine_1, other_1, totals[1], product, scales, interp_v),
            )
            totals = (total_0, total_1)
    blocks = call_term(
        last_kernel,
        blocks_shape,
        *(mine_1, other_1, total_0, totals[1], product, scales, interp_v),
    )
    returned = lax.all_to_all(blocks, ("y", "core"), 0, 0, tiled=True, axis_index_groups=CHOL_RANKS)
    return call_end(returned), force_bias


def solution(mesh):
    fine = Mesh(mesh.devices.reshape(NZ, NX, NY, NC), ("z", "x", "y", "core"))
    walk, chol = ("z", "x"), ("y", "core")
    return jax.shard_map(
        on_device,
        mesh=fine,
        in_specs=(
            P(walk, None, chol),
            P(walk, None, None),
            P(None, chol),
            P(None, chol),
            P(chol, walk),
            P(None, walk),
        ),
        out_specs=(P(walk, None, chol), P(None, walk)),
        check_vma=False,
    )
```
